16 devices in a mesh: dp: 2 (over y, z), ws: 8 (over x, core).
Axes of the slice: x: 4, y: 2, z: 1, core: 2. Of those that a mesh axis runs over, the one named last changes fastest.
The devices are a block of a 4x4x8 slice.
Arguments:
- hidden: bfloat16 [256, 768], P(('dp', 'ws')), parts along dimension 0
- self_k: bfloat16 [256, 12, 384, 64], P(('dp', 'ws')), parts along dimension 0
- self_v: bfloat16 [256, 12, 384, 64], P(('dp', 'ws')), parts along dimension 0
- cross_k: bfloat16 [256, 12, 1024, 64], P(('dp', 'ws')), parts along dimension 0
- cross_v: bfloat16 [256, 12, 1024, 64], P(('dp', 'ws')), parts along dimension 0
- positions: int32 [256], P(('dp', 'ws')), parts along dimension 0
- enc_mask: int32 [256, 1024], P(('dp', 'ws')), parts along dimension 0
- rel_bias: float32 [12, 384], replicated
- expert_idx: int32 [256], P(('dp', 'ws')), parts along dimension 0
- ln_self: float32 [768], replicated
- ln_cross: float32 [768], replicated
- ln_ffn: float32 [768], replicated
- wq_self: bfloat16 [768, 768], P(None, 'ws')
- wk_self: bfloat16 [768, 768], P(None, 'ws')
- wv_self: bfloat16 [768, 768], P(None, 'ws')
- wo_self: bfloat16 [768, 768], P(None, 'ws')
- wq_cross: bfloat16 [768, 768], P(None, 'ws')
- wo_cross: bfloat16 [768, 768], P(None, 'ws')
- w_router: float32 [768, 8], P(None, 'ws')
- w_in: bfloat16 [8, 768, 3072], P(None, None, 'ws')
- w_out: bfloat16 [8, 3072, 768], P(None, 'ws')
Outputs:
- output 1: bfloat16 [256, 768], P(('dp', 'ws')), parts along dimension 0
- output 2: bfloat16 [256, 12, 384, 64], P(('dp', 'ws')), parts along dimension 0
- output 3: bfloat16 [256, 12, 384, 64], P(('dp', 'ws')), parts along dimension 0
There are 2 independent parts. The reference program is written for one: setup_inputs(seed, part) draws one part's arguments, and reference() takes and returns one part's arrays. A program takes and returns all parts, laid end to end along the dimension named above; an argument that names none is the same for every part.
All inputs are finite; a program needn't handle non-finite values.
Results may differ from the reference program's by a relative error of at most 0.0110425.
Values are sent between devices in bfloat16 or wider.
A program may use at most 768 MiB of HBM per device.

```python
import jax
import jax.numpy as jnp
from jax import lax

D_MODEL = 768
NUM_HEADS = 12
HEAD_DIM = 64
D_FF = 3072
EXPERTS = 8
CACHE_LEN = 384
SRC_LEN = 1024
GROUP_ROWS = 128

ATTN_WIDTH = NUM_HEADS * HEAD_DIM
CAPACITY = (2 * GROUP_ROWS + EXPERTS - 1) // EXPERTS
EPSILON = 1e-6
NEG_BIG = -1e30


def scaled_normal(key, shape, scale):
    return (jax.random.normal(key, shape, jnp.float32) * scale).astype(jnp.bfloat16)


def setup_inputs(seed: int = 0, part: int = 0) -> dict:
    base_key = jax.random.key(seed)
    shared = jax.random.split(base_key, 13)
    part_keys = jax.random.split(jax.random.fold_in(base_key, part), 12)
    row_ids = jnp.arange(GROUP_ROWS)
    cache_shape = (GROUP_ROWS, NUM_HEADS, CACHE_LEN, HEAD_DIM)
    src_shape = (GROUP_ROWS, NUM_HEADS, SRC_LEN, HEAD_DIM)
    hidden = scaled_normal(part_keys[0], (GROUP_ROWS, D_MODEL), 1.0)
    self_k = scaled_normal(part_keys[1], cache_shape, 1.0)
    self_v = scaled_normal(part_keys[2], cache_shape, 1.0)
    cross_k = scaled_normal(part_keys[3], src_shape, 1.0)
    cross_v = scaled_normal(part_keys[4], src_shape, 1.0)
    positions = jax.random.randint(part_keys[5], (GROUP_ROWS,), 0, CACHE_LEN)
    last_row = jax.random.randint(part_keys[6], (), 0, GROUP_ROWS)
    positions = jnp.where(row_ids == last_row, CACHE_LEN - 1, positions).astype(jnp.int32)
    src_lens = jax.random.randint(part_keys[7], (GROUP_ROWS,), 1, SRC_LEN + 1)
    full_row = jax.random.randint(part_keys[8], (), 0, GROUP_ROWS)
    src_lens = jnp.where(row_ids == full_row, SRC_LEN, src_lens)
    enc_mask = (jnp.arange(SRC_LEN)[None, :] < src_lens[:, None]).astype(jnp.int32)
    hot_expert = jax.random.randint(part_keys[9], (), 0, EXPERTS)
    free_pick = jax.random.randint(part_keys[10], (GROUP_ROWS,), 0, EXPERTS)
    row_order = jax.random.permutation(part_keys[11], GROUP_ROWS)
    hot_rows = jnp.zeros((GROUP_ROWS,), jnp.int32).at[row_order[:CAPACITY + 1]].set(1)
    expert_idx = jnp.where(hot_rows == 1, hot_expert, free_pick).astype(jnp.int32)
    return {
        'hidden': hidden,
        'self_k': self_k,
        'self_v': self_v,
        'cross_k': cross_k,
        'cross_v': cross_v,
        'positions': positions,
        'enc_mask': enc_mask,
        'rel_bias': jax.random.normal(shared[0], (NUM_HEADS, CACHE_LEN), jnp.float32),
        'expert_idx': expert_idx,
        'ln_self': jax.random.uniform(shared[1], (D_MODEL,), jnp.float32, 0.5, 1.5),
        'ln_cross': jax.random.uniform(shared[2], (D_MODEL,), jnp.float32, 0.5, 1.5),
        'ln_ffn': jax.random.uniform(shared[3], (D_MODEL,), jnp.float32, 0.5, 1.5),
        'wq_self': scaled_normal(shared[4], (D_MODEL, ATTN_WIDTH), 1.5 * (D_MODEL * HEAD_DIM) ** -0.5),
        'wk_self': scaled_normal(shared[5], (D_MODEL, ATTN_WIDTH), D_MODEL ** -0.5),
        'wv_self': scaled_normal(shared[6], (D_MODEL, ATTN_WIDTH), D_MODEL ** -0.5),
        'wo_self': scaled_normal(shared[7], (ATTN_WIDTH, D_MODEL), ATTN_WIDTH ** -0.5),
        'wq_cross': scaled_normal(shared[8], (D_MODEL, ATTN_WIDTH), 1.5 * (D_MODEL * HEAD_DIM) ** -0.5),
        'wo_cross': scaled_normal(shared[9], (ATTN_WIDTH, D_MODEL), ATTN_WIDTH ** -0.5),
        'w_router': jax.random.normal(shared[10], (D_MODEL, EXPERTS), jnp.float32) * D_MODEL ** -0.5,
        'w_in': scaled_normal(shared[11], (EXPERTS, D_MODEL, D_FF), D_MODEL ** -0.5),
        'w_out': scaled_normal(shared[12], (EXPERTS, D_FF, D_MODEL), (EXPERTS / D_FF) ** 0.5),
    }


def rms_norm(hidden, scale):
    hid_f32 = hidden.astype(jnp.float32)
    inv_rms = lax.rsqrt(jnp.mean(hid_f32 * hid_f32, axis=-1, keepdims=True) + EPSILON)
    return (hid_f32 * inv_rms * scale).astype(jnp.bfloat16)


def attend_row(row_args):
    queries, cache_keys, cache_vals, score_bias = row_args
    scores = jnp.einsum('hd,hld->hl', queries.astype(jnp.float32), cache_keys.astype(jnp.float32)) + score_bias
    attn_probs = jax.nn.softmax(scores, axis=-1).astype(jnp.bfloat16)
    context = jnp.einsum('hl,hld->hd', attn_probs.astype(jnp.float32), cache_vals.astype(jnp.float32))
    return context.astype(jnp.bfloat16)


def project(x_norm, weight):
    return jnp.dot(x_norm, weight, preferred_element_type=jnp.float32).astype(jnp.bfloat16)


def reference(hidden, self_k, self_v, cross_k, cross_v, positions, enc_mask, rel_bias, expert_idx,
              ln_self, ln_cross, ln_ffn, wq_self, wk_self, wv_self, wo_self, wq_cross, wo_cross,
              w_router, w_in, w_out):
    head_shape = (GROUP_ROWS, NUM_HEADS, HEAD_DIM)
    x_norm = rms_norm(hidden, ln_self)
    queries = project(x_norm, wq_self).reshape(head_shape)
    k_new = project(x_norm, wk_self).reshape(head_shape)
    v_new = project(x_norm, wv_self).reshape(head_shape)
    distance = positions[:, None] - jnp.arange(CACHE_LEN)[None, :]
    write_mask = (distance == 0)[:, None, :, None]
    new_self_k = jnp.where(write_mask, k_new[:, :, None, :], self_k)
    new_self_v = jnp.where(write_mask, v_new[:, :, None, :], self_v)
    pos_bias = jnp.take(rel_bias, jnp.clip(distance, 0, CACHE_LEN - 1), axis=1)
    pos_bias = jnp.where(distance[None] >= 0, pos_bias, NEG_BIG).transpose(1, 0, 2)
    context = lax.map(attend_row, (queries, new_self_k, new_self_v, pos_bias))
    attn_out = jnp.dot(context.reshape(GROUP_ROWS, ATTN_WIDTH), wo_self, preferred_element_type=jnp.float32)
    after_self = (hidden.astype(jnp.float32) + attn_out).astype(jnp.bfloat16)

    x_norm = rms_norm(after_self, ln_cross)
    queries = project(x_norm, wq_cross).reshape(head_shape)
    mask_bias = jnp.where(enc_mask == 1, 0.0, NEG_BIG)[:, None, :]
    context = lax.map(attend_row, (queries, cross_k, cross_v, mask_bias))
    attn_out = jnp.dot(context.reshape(GROUP_ROWS, ATTN_WIDTH), wo_cross, preferred_element_type=jnp.float32)
    after_cross = (after_self.astype(jnp.float32) + attn_out).astype(jnp.bfloat16)

    x_norm = rms_norm(after_cross, ln_ffn)
    logits = jnp.dot(x_norm.astype(jnp.float32), w_router, precision=lax.Precision.HIGHEST,
                     preferred_element_type=jnp.float32)
    router_probs = jax.nn.softmax(logits, axis=-1)
    chosen = jnp.arange(EXPERTS)[None, :] == expert_idx[:, None]
    gate_val = jnp.sum(jnp.where(chosen, router_probs, 0.0), axis=-1)
    row_ids = jnp.arange(GROUP_ROWS)
    earlier = (expert_idx[None, :] == expert_idx[:, None]) & (row_ids[None, :] < row_ids[:, None])
    slot_idx = jnp.sum(earlier.astype(jnp.int32), axis=1)
    keep_gate = jnp.where(slot_idx < CAPACITY, gate_val, 0.0)

    def expert_row(row_args):
        x_row, expert = row_args
        ffn_hidden = jnp.dot(x_row[None, :], w_in[expert], preferred_element_type=jnp.float32)
        ffn_hidden = jax.nn.relu(ffn_hidden).astype(jnp.bfloat16)
        ffn_out = jnp.dot(ffn_hidden, w_out[expert], preferred_element_type=jnp.float32)
        return ffn_out.astype(jnp.bfloat16)[0]

    expert_out = lax.map(expert_row, (x_norm, expert_idx))
    hidden_out = (after_cross.astype(jnp.float32) + expert_out.astype(jnp.float32) * keep_gate[:, None]).astype(jnp.bfloat16)
    return (hidden_out, new_self_k, new_self_v)
```

```python
import functools
import jax
import jax.numpy as jnp
from jax import lax
from jax.experimental import pallas as pl
from jax.experimental.pallas import tpu as pltpu
from jax.sharding import PartitionSpec as P

EPSILON = 1e-6
NEG_BIG = -1e30
MESH = pl.DeviceIdType.MESH
F32 = jnp.float32
BF16 = jnp.bfloat16
CHUNK = 256
GROUP = 4
SLOTS = 40
VMEM_LIMIT = 63 * 1024 * 1024

vmem = functools.partial(pl.BlockSpec, memory_space=pltpu.VMEM)
smem = functools.partial(pl.BlockSpec, memory_space=pltpu.SMEM)
hbm = functools.partial(pl.BlockSpec, memory_space=pl.ANY)


def rms(hid_f32, scale):
    inv = lax.rsqrt(jnp.mean(hid_f32 * hid_f32, axis=-1, keepdims=True) + EPSILON)
    return (hid_f32 * inv * scale).astype(BF16)


def dot_nn(a, b):
    return lax.dot_general(a, b, (((1,), (0,)), ((), ())), preferred_element_type=F32)


def dot_nt(a, b):
    return lax.dot_general(a, b, (((1,), (1,)), ((), ())), preferred_element_type=F32)


def remote(src, dst, send, recv, dev):
    return pltpu.make_async_remote_copy(src_ref=src, dst_ref=dst, send_sem=send, recv_sem=recv,
                                        device_id={"ws": dev}, device_id_type=MESH)


def enter(me, n):
    barrier = pltpu.get_barrier_semaphore()
    for d in range(1, n):
        pl.semaphore_signal(barrier, inc=1, device_id={"ws": lax.rem(me + d, n)}, device_id_type=MESH)
    pl.semaphore_wait(barrier, n - 1)


def rows_of(ref, i, rows):
    return ref.at[pl.ds(pl.multiple_of(i * rows, rows), rows)]


def head_mask(heads_pad, width, head_dim):
    sub = lax.broadcasted_iota(jnp.int32, (heads_pad, width), 0) * head_dim
    lane = lax.broadcasted_iota(jnp.int32, (heads_pad, width), 1)
    return (lane >= sub) & (lane < sub + head_dim)


def softmax_rows(s):
    e = jnp.exp(s - jnp.max(s, axis=-1, keepdims=True))
    return e / jnp.sum(e, axis=-1, keepdims=True)


def self_kernel(n, heads, pos_ref, hid_ref, mask_ref, relb_ref, ln1_ref, ln2_ref, wq_ref, wk_ref, wv_ref,
                wo_ref, wqc_ref, woc_ref, sk_ref, sv_ref,
                qc_out, h1_out, kn_out, vn_out, lens_out, woc_out,
                hall, stage, got, kbuf, vbuf, wall, q_s, k_s, v_s, qbd, snew, ctx_s, relrev,
                ksem, vsem, hsend, hrecv, asend, arecv, wsend, wrecv, fsend, frecv):
    me = lax.axis_index("ws")
    rows, model = hid_ref.shape
    cols = wq_ref.shape[0]
    width = cols * n
    cache_len = sk_ref.shape[2]
    heads_pad = qbd.shape[0] // rows
    head_dim = width // heads
    chips = n // 2

    for b in range(rows):
        pltpu.make_async_copy(sk_ref.at[b], kbuf.at[b], ksem.at[b]).start()
        pltpu.make_async_copy(sv_ref.at[b], vbuf.at[b], vsem.at[b]).start()

    stage[...] = jnp.zeros_like(stage)
    enter(me, n)

    def h_copy(src, dev):
        return remote(hid_ref, rows_of(hall, src, rows), hsend.at[dev], hrecv.at[src], dev)

    for d in range(1, n):
        h_copy(me, lax.rem(me + d, n)).start()

    chip, core = me // 2, lax.rem(me, 2)
    wshards = (wo_ref, wqc_ref, woc_ref)

    def w_copy(t, src, dev):
        return remote(wshards[t], rows_of(wall.at[t], src, cols), wsend.at[t, dev], wrecv.at[t, src], dev)

    def f_copy(t, src, dev):
        piece = rows_of(wall.at[t], src, cols)
        return remote(piece, piece, fsend.at[t, src], frecv.at[t, src], dev)

    def across(d):
        return lax.rem(chip + d, chips) * 2 + core

    def w_start(t):
        for d in range(1, chips):
            w_copy(t, me, across(d)).start()
        w_copy(t, me, me + 1 - 2 * core).start()

    def w_forward(t):
        for d in range(1, chips):
            src = across(d)
            w_copy(t, src, me).wait_recv()
            f_copy(t, src, me + 1 - 2 * core).start()

    def w_finish(t):
        w_copy(t, me + 1 - 2 * core, me).wait_recv()
        for d in range(1, chips):
            f_copy(t, across(d) + 1 - 2 * core, me).wait_recv()

    w_start(0)
    hall[pl.ds(pl.multiple_of(me * rows, rows), rows), :] = hid_ref[...]
    for t in range(3):
        wall[t, pl.ds(pl.multiple_of(me * cols, cols), cols), :] = wshards[t][...]

    rb = relb_ref[...]
    rev = (lax.broadcasted_iota(jnp.int32, (cache_len, cache_len), 0)
           + lax.broadcasted_iota(jnp.int32, (cache_len, cache_len), 1) == cache_len - 1).astype(BF16)
    hi = rb.astype(BF16)
    mid = (rb - hi.astype(F32)).astype(BF16)
    low = (rb - hi.astype(F32) - mid.astype(F32)).astype(BF16)
    relrev[...] = jnp.zeros_like(relrev)
    relrev[0:heads, :] = dot_nn(hi, rev) + dot_nn(mid, rev) + dot_nn(low, rev)
    lens_out[...] = jnp.broadcast_to(
        jnp.sum(mask_ref[...].astype(F32), axis=-1, keepdims=True), lens_out.shape).astype(jnp.int32)

    for d in range(1, n):
        h_copy(lax.rem(me + n - d, n), me).wait_recv()
    x = rms(hall[...].astype(F32), ln1_ref[...])
    for i, w in enumerate((wq_ref, wk_ref, wv_ref)):
        y = dot_nt(x, w[...]).astype(BF16)
        for j in range(n):
            stage[j, :, i * 128:i * 128 + cols] = y[j * rows:(j + 1) * rows, :]

    def a_copy(src, dev):
        return remote(stage.at[dev], got.at[src], asend.at[dev], arecv.at[src], dev)

    for d in range(1, n):
        a_copy(me, lax.rem(me + d, n)).start()
    got[me] = stage[me]
    w_start(1)
    w_start(2)
    for d in range(1, n):
        a_copy(lax.rem(me + n - d, n), me).wait_recv()

    lane = lax.broadcasted_iota(jnp.int32, (rows, 128), 1)
    for i, dst in enumerate((q_s, k_s, v_s)):
        tiles = [None] * (width // 128)
        for s in range(n):
            piece = got[s, :, i * 128:(i + 1) * 128].astype(F32)
            t, r = divmod(s * cols, 128)
            if r:
                piece = pltpu.roll(piece, r, axis=1)
            ends = ((t, r, min(128, r + cols)), (t + 1, 0, r + cols - 128))
            for tile, lo, hi_ in ends:
                if hi_ > lo:
                    base = jnp.zeros((rows, 128), F32) if tiles[tile] is None else tiles[tile]
                    tiles[tile] = jnp.where((lane >= lo) & (lane < hi_), piece, base)
        for t, tile in enumerate(tiles):
            dst[:, t * 128:(t + 1) * 128] = tile
    kn_out[...] = k_s[...].astype(BF16)
    vn_out[...] = v_s[...].astype(BF16)

    diag = head_mask(heads_pad, width, head_dim)
    for b in range(rows):
        qbd[b * heads_pad:(b + 1) * heads_pad, :] = jnp.where(
            diag, jnp.broadcast_to(q_s[b:b + 1, :], diag.shape), 0.0).astype(BF16)
    cross = dot_nt(qbd[...], k_s[...].astype(BF16))
    own = (lax.broadcasted_iota(jnp.int32, cross.shape, 0) // heads_pad
           == lax.broadcasted_iota(jnp.int32, cross.shape, 1))
    snew[...] = jnp.broadcast_to(jnp.sum(jnp.where(own, cross, 0.0), axis=-1, keepdims=True), snew.shape)

    col = lax.broadcasted_iota(jnp.int32, (heads_pad, cache_len), 1)

    def attend(b):
        pos = pos_ref[b]
        head_rows = pl.ds(pl.multiple_of(b * heads_pad, heads_pad), heads_pad)
        pltpu.make_async_copy(sk_ref.at[b], kbuf.at[b], ksem.at[b]).wait()
        pltpu.make_async_copy(sv_ref.at[b], vbuf.at[b], vsem.at[b]).wait()
        s = dot_nn(qbd[head_rows, :], kbuf[b])
        s = jnp.where(col == pos, snew[head_rows, 0:1], s)
        bias = pltpu.roll(relrev[...], lax.rem(pos + 1, cache_len), axis=1)
        s = jnp.where(col <= pos, s + bias, NEG_BIG)
        p = softmax_rows(s).astype(BF16).astype(F32)
        pnew = jnp.sum(jnp.where(col == pos, p, 0.0), axis=-1, keepdims=True)
        pold = jnp.where(col == pos, 0.0, p).astype(BF16)
        c = dot_nt(pold, vbuf[b]) + pnew * v_s[pl.ds(b, 1), :]
        ctx_s[pl.ds(b, 1), :] = jnp.sum(jnp.where(diag, c, 0.0), axis=0, keepdims=True)

    quarter = rows // 4

    def part(lo):
        def body(i, carry):
            for r in range(2):
                attend(i * 2 + r)
            return carry
        lax.fori_loop(lo * quarter // 2, (lo + 1) * quarter // 2, body, 0)

    part(0)
    w_forward(0)
    part(1)
    part(2)
    w_forward(1)
    part(3)
    w_forward(2)

    w_finish(0)
    h1 = (hid_ref[...].astype(F32) + dot_nt(ctx_s[...].astype(BF16), wall[0])).astype(BF16)
    h1_out[...] = h1
    w_finish(1)
    x = rms(h1.astype(F32), ln2_ref[...])
    qc_out[...] = dot_nt(x, wall[1])
    w_finish(2)
    pltpu.sync_copy(wall.at[2], woc_out)

    for d in range(1, n):
        h_copy(me, lax.rem(me + d, n)).wait_send()
        a_copy(me, lax.rem(me + d, n)).wait_send()
    for t in range(3):
        for d in range(1, chips):
            w_copy(t, me, across(d)).wait_send()
            f_copy(t, across(d), me + 1 - 2 * core).wait_send()
        w_copy(t, me, me + 1 - 2 * core).wait_send()


def cross_kernel(heads, pos_ref, lens_ref, qc_ref, kn_ref, vn_ref, h1_ref, ln3_ref, woc_ref, ck_ref, cv_ref,
                 sk_ref, sv_ref, h2_out, x2_out, nk_out, nv_out,
                 ring, kbuf, vbuf, scores, probs, qbd, qf_s, kt_s, vt_s, ctx_s, item_row, item_col,
                 rsem, ksem, vsem, kout, vout):
    rows, width = qc_ref.shape
    src_len = ck_ref.shape[2]
    heads_pad = qbd.shape[1]
    head_dim = width // heads
    cap = item_row.shape[0]
    diag = head_mask(heads_pad, width, head_dim)

    total = 0
    for b in range(rows):
        count = (lens_ref[b, 0] + CHUNK - 1) // CHUNK

        def put(c, carry, b=b, total=total):
            item_row[total + c] = b
            item_col[total + c] = c
            return carry

        lax.fori_loop(0, count, put, 0)
        total = total + count
    groups = (total + GROUP - 1) // GROUP
    padded = groups * GROUP

    def fill(i, carry):
        item_row[i] = rows
        item_col[i] = 0
        return carry

    lax.fori_loop(total, padded, fill, 0)

    def fetch(s):
        slot = lax.rem(s, SLOTS)

        def start(src, i):
            b = jnp.minimum(item_row[i], rows - 1)
            c = pl.multiple_of(item_col[i] * CHUNK, CHUNK)
            pltpu.make_async_copy(src.at[b, :, pl.ds(c, CHUNK)], ring.at[slot], rsem.at[slot]).start()

        @pl.when(s < padded)
        def _():
            start(ck_ref, s)

        @pl.when((s >= padded) & (s < 2 * padded))
        def _():
            start(cv_ref, s - padded)

    def arrive(s):
        slot = lax.rem(s, SLOTS)
        pltpu.make_async_copy(ck_ref.at[0, :, pl.ds(0, CHUNK)], ring.at[slot], rsem.at[slot]).wait()
        return slot

    lax.fori_loop(0, SLOTS, lambda s, c: (fetch(s), c)[1], 0)
    for b in range(rows):
        pltpu.make_async_copy(sk_ref.at[b], kbuf.at[b], ksem.at[b]).start()
        pltpu.make_async_copy(sv_ref.at[b], vbuf.at[b], vsem.at[b]).start()

    qf_s[...] = qc_ref[...]
    for b in range(rows):
        qbd[b] = jnp.where(diag, jnp.broadcast_to(qf_s[b:b + 1, :], diag.shape), 0.0).astype(BF16)
    qbd[rows] = jnp.zeros_like(qbd[rows])
    ctx_s[...] = jnp.zeros_like(ctx_s)
    kt_s[...] = jnp.transpose(kn_ref[...].astype(F32))
    vt_s[...] = jnp.transpose(vn_ref[...].astype(F32))

    def score_group(g, carry):
        for r in range(GROUP):
            i = g * GROUP + r
            slot = arrive(i)
            b = item_row[i]
            c = pl.multiple_of(item_col[i] * CHUNK, CHUNK)
            scores[b, :, pl.ds(c, CHUNK)] = dot_nn(qbd[b], ring[slot])
        for r in range(GROUP):
            fetch(g * GROUP + r + SLOTS)
        return carry

    lax.fori_loop(0, groups, score_group, 0)

    col = lax.broadcasted_iota(jnp.int32, (heads_pad, src_len), 1)

    def soft(i, carry):
        for r in range(4):
            b = i * 4 + r
            s = jnp.where(col < lens_ref[b, 0], scores[b], NEG_BIG)
            probs[b] = softmax_rows(s).astype(BF16)
        return carry

    lax.fori_loop(0, rows // 4, soft, 0)
    probs[rows] = jnp.zeros_like(probs[rows])

    lane = lax.broadcasted_iota(jnp.int32, (width, 128), 1)
    for b in range(rows):
        pos = pos_ref[b]
        tile = pl.ds(pl.multiple_of(pos // 128 * 128, 128), 128)
        here = lane == lax.rem(pos, 128)
        for src, buf, sem, new, dst, osem in ((sk_ref, kbuf, ksem, kt_s, nk_out, kout),
                                              (sv_ref, vbuf, vsem, vt_s, nv_out, vout)):
            pltpu.make_async_copy(src.at[b], buf.at[b], sem.at[b]).wait()
            old = buf[b, :, tile].astype(F32)
            buf[b, :, tile] = jnp.where(here, new[:, b:b + 1], old).astype(BF16)
            pltpu.make_async_copy(buf.at[b], dst.at[b], osem.at[b]).start()

    def value_group(g, carry):
        parts = []
        for r in range(GROUP):
            i = g * GROUP + r
            slot = arrive(padded + i)
            b = item_row[i]
            c = pl.multiple_of(item_col[i] * CHUNK, CHUNK)
            full = dot_nt(probs[b, :, pl.ds(c, CHUNK)], ring[slot])
            parts.append((b, jnp.sum(jnp.where(diag, full, 0.0), axis=0, keepdims=True)))
        for b, v in parts:
            ctx_s[pl.ds(b, 1), :] = ctx_s[pl.ds(b, 1), :] + v
        for r in range(GROUP):
            fetch(padded + g * GROUP + r + SLOTS)
        return carry

    lax.fori_loop(0, groups, value_group, 0)

    h1 = h1_ref[...].astype(F32)
    h2 = (h1 + dot_nt(ctx_s[0:rows, :].astype(BF16), woc_ref[...])).astype(BF16)
    h2_out[...] = h2
    x2_out[...] = rms(h2.astype(F32), ln3_ref[...])
    for b in range(rows):
        pltpu.make_async_copy(kbuf.at[b], nk_out.at[b], kout.at[b]).wait()
        pltpu.make_async_copy(vbuf.at[b], nv_out.at[b], vout.at[b]).wait()


def ffn_kernel(n, x2_ref, h2_ref, idx_ref, router_ref, win_ref, wout_ref, out_ref,
               xall, idx_s, iall, rall, win, wout, act, stage, got,
               isem, osem, xsend, xrecv, jsend, jrecv, rsend, rrecv, ysend, yrecv):
    me = lax.axis_index("ws")
    rows, model = x2_ref.shape
    experts, _, hidden = win_ref.shape
    group = rows * n
    capacity = (2 * group + experts - 1) // experts

    for e in range(experts):
        pltpu.make_async_copy(win_ref.at[e], win.at[e], isem.at[e]).start()
    for e in range(experts):
        pltpu.make_async_copy(wout_ref.at[e], rows_of(wout, e, hidden), osem.at[e]).start()

    eye = (lax.broadcasted_iota(jnp.int32, (rows, rows), 0) == lax.broadcasted_iota(jnp.int32, (rows, rows), 1))
    idx_col = jnp.sum(jnp.where(eye, jnp.broadcast_to(idx_ref[...].astype(F32), (rows, rows)), 0.0),
                      axis=-1, keepdims=True)
    idx_s[...] = jnp.broadcast_to(idx_col, idx_s.shape)
    enter(me, n)

    def x_copy(src, dev):
        return remote(x2_ref, rows_of(xall, src, rows), xsend.at[dev], xrecv.at[src], dev)

    def i_copy(src, dev):
        return remote(idx_s, rows_of(iall, src, rows), jsend.at[dev], jrecv.at[src], dev)

    def r_copy(src, dev):
        return remote(router_ref, rall.at[src], rsend.at[dev], rrecv.at[src], dev)

    for copy in (x_copy, i_copy, r_copy):
        for d in range(1, n):
            copy(me, lax.rem(me + d, n)).start()
    mine = pl.ds(pl.multiple_of(me * rows, rows), rows)
    xall[mine, :] = x2_ref[...]
    iall[mine, :] = idx_s[...]
    rall[me] = router_ref[...]
    for copy in (x_copy, i_copy, r_copy):
        for d in range(1, n):
            copy(lax.rem(me + n - d, n), me).wait_recv()

    x = xall[...]
    chosen = iall[:, 0:1]
    for e in range(experts):
        pltpu.make_async_copy(win_ref.at[e], win.at[e], isem.at[e]).wait()
        u = jnp.maximum(dot_nn(x, win[e]), 0.0)
        act[:, e * hidden:(e + 1) * hidden] = jnp.where(chosen == float(e), u, 0.0).astype(BF16)
    for e in range(experts):
        pltpu.make_async_copy(wout_ref.at[e], rows_of(wout, e, hidden), osem.at[e]).wait()

    halves, _, _, span = stage.shape

    def y_copy(h, src, dev):
        return remote(stage.at[h, dev], got.at[h, src], ysend.at[h, dev], yrecv.at[h, src], dev)

    for h in range(halves):
        y = dot_nn(act[...], wout[:, h * span:(h + 1) * span])
        for j in range(n):
            stage[h, j] = y[j * rows:(j + 1) * rows, :]
        for d in range(1, n):
            y_copy(h, me, lax.rem(me + d, n)).start()
        got[h, me] = stage[h, me]

    xr = x2_ref[...].astype(F32)
    logits = [jnp.sum(xr * rall[e], axis=-1, keepdims=True) for e in range(experts)]
    top = functools.reduce(jnp.maximum, logits)
    exps = [jnp.exp(v - top) for v in logits]
    denom = functools.reduce(jnp.add, exps)
    my_idx = idx_s[:, 0:1]
    gate = functools.reduce(jnp.add, [jnp.where(my_idx == float(e), exps[e] / denom, 0.0) for e in range(experts)])
    others = jnp.transpose(iall[...])[0:rows, :]
    row = me * rows + lax.broadcasted_iota(jnp.int32, (rows, group), 0)
    col = lax.broadcasted_iota(jnp.int32, (rows, group), 1)
    slot = jnp.sum(jnp.where((others == my_idx) & (col < row), 1.0, 0.0), axis=-1, keepdims=True)
    gate = jnp.where(slot < float(capacity), gate, 0.0)

    for h in range(halves):
        for d in range(1, n):
            y_copy(h, lax.rem(me + n - d, n), me).wait_recv()
        y = functools.reduce(jnp.add, [got[h, s] for s in range(n)]).astype(BF16).astype(F32)
        part = slice(h * span, (h + 1) * span)
        out_ref[:, part] = (h2_ref[:, part].astype(F32) + y * gate).astype(BF16)

    for d in range(1, n):
        dev = lax.rem(me + d, n)
        for copy in (x_copy, i_copy, r_copy):
            copy(me, dev).wait_send()
        for h in range(halves):
            y_copy(h, me, dev).wait_send()


def solution(mesh):
    n = mesh.shape['ws']
    row_axes = ('dp', 'ws')
    row_vec = P(row_axes)
    row_mat = P(row_axes, None)
    cache_spec = P(row_axes, None, None, None)
    col_split = P(None, 'ws')
    in_specs = (row_mat, cache_spec, cache_spec, cache_spec, cache_spec, row_vec, row_mat, P(None, None), row_vec,
                P(None), P(None), P(None), col_split, col_split, col_split, col_split, col_split, col_split,
                col_split, P(None, None, 'ws'), P(None, 'ws', None))
    out_specs = (row_mat, cache_spec, cache_spec)
    dma = pltpu.SemaphoreType.DMA

    def decoder_block(hidden, self_k, self_v, cross_k, cross_v, positions, enc_mask, rel_bias, expert_idx,
                      ln_self, ln_cross, ln_ffn, wq_self, wk_self, wv_self, wo_self, wq_cross, wo_cross,
                      w_router, w_in, w_out):
        rows, model = hidden.shape
        _, heads, cache_len, head_dim = self_k.shape
        src_len = cross_k.shape[2]
        width = heads * head_dim
        cols = wq_self.shape[1]
        heads_pad = (heads + 15) // 16 * 16
        experts, _, ff = w_in.shape

        def flat(cache):
            return jnp.swapaxes(cache, 2, 3).reshape(rows, width, cache.shape[2])

        def unflat(cache):
            return jnp.swapaxes(cache.reshape(rows, heads, head_dim, cache.shape[2]), 2, 3)

        sds = jax.ShapeDtypeStruct
        sk, sv, ck, cv = flat(self_k), flat(self_v), flat(cross_k), flat(cross_v)
        qc, h1, kn, vn, lens, woc = pl.pallas_call(
            functools.partial(self_kernel, n, heads),
            name="self_attention",
            out_shape=(sds((rows, width), F32), sds((rows, model), BF16), sds((rows, width), BF16),
                       sds((rows, width), BF16), sds((rows, 128), jnp.int32), sds((model, width), BF16)),
            in_specs=[smem()] + [vmem()] * 11 + [hbm(), hbm()],
            out_specs=tuple([vmem()] * 5 + [hbm()]),
            scratch_shapes=[
                pltpu.VMEM((rows * n, model), BF16), pltpu.VMEM((n, rows, 384), BF16),
                pltpu.VMEM((n, rows, 384), BF16), pltpu.VMEM((rows, width, cache_len), BF16),
                pltpu.VMEM((rows, width, cache_len), BF16), pltpu.VMEM((3, width, model), BF16),
                pltpu.VMEM((rows, width), F32), pltpu.VMEM((rows, width), F32), pltpu.VMEM((rows, width), F32),
                pltpu.VMEM((rows * heads_pad, width), BF16), pltpu.VMEM((rows * heads_pad, 128), F32),
                pltpu.VMEM((rows, width), F32), pltpu.VMEM((heads_pad, cache_len), F32),
                dma((rows,)), dma((rows,)), dma((n,)), dma((n,)), dma((n,)), dma((n,)),
                dma((3, n)), dma((3, n)), dma((3, n)), dma((3, n))],
            compiler_params=pltpu.CompilerParams(collective_id=0, has_side_effects=True,
                                                 vmem_limit_bytes=VMEM_LIMIT),
        )(positions, hidden, enc_mask, rel_bias, ln_self.reshape(1, -1), ln_cross.reshape(1, -1),
          wq_self.T, wk_self.T, wv_self.T, wo_self.T, wq_cross.T, wo_cross.T, sk, sv)

        items = rows * (src_len // CHUNK) + GROUP
        h2, x2, nk, nv = pl.pallas_call(
            functools.partial(cross_kernel, heads),
            name="cross_attention",
            out_shape=(sds((rows, model), BF16), sds((rows, model), BF16), sds(sk.shape, BF16), sds(sv.shape, BF16)),
            in_specs=[smem(), smem()] + [vmem()] * 6 + [hbm()] * 4,
            out_specs=(vmem(), vmem(), hbm(), hbm()),
            scratch_shapes=[
                pltpu.VMEM((SLOTS, width, CHUNK), BF16), pltpu.VMEM((rows, width, cache_len), BF16),
                pltpu.VMEM((rows, width, cache_len), BF16), pltpu.VMEM((rows + 1, heads_pad, src_len), F32),
                pltpu.VMEM((rows + 1, heads_pad, src_len), BF16), pltpu.VMEM((rows + 1, heads_pad, width), BF16),
                pltpu.VMEM((rows, width), F32), pltpu.VMEM((width, rows), F32), pltpu.VMEM((width, rows), F32),
                pltpu.VMEM((rows + 8, width), F32), pltpu.SMEM((items,), jnp.int32), pltpu.SMEM((items,), jnp.int32),
                dma((SLOTS,)), dma((rows,)), dma((rows,)), dma((rows,)), dma((rows,))],
            compiler_params=pltpu.CompilerParams(vmem_limit_bytes=VMEM_LIMIT),
        )(positions, lens, qc, kn, vn, h1, ln_ffn.reshape(1, -1), woc, ck, cv, sk, sv)

        halves = 2
        out = pl.pallas_call(
            functools.partial(ffn_kernel, n),
            name="switch_ffn",
            out_shape=sds((rows, model), BF16),
            in_specs=[vmem()] * 4 + [hbm(), hbm()],
            out_specs=vmem(),
            scratch_shapes=[
                pltpu.VMEM((rows * n, model), BF16), pltpu.VMEM((rows, 128), F32), pltpu.VMEM((rows * n, 128), F32),
                pltpu.VMEM((n, 1, model), F32), pltpu.VMEM(w_in.shape, BF16), pltpu.VMEM((experts * w_out.shape[1], model), BF16),
                pltpu.VMEM((rows * n, experts * ff), BF16), pltpu.VMEM((halves, n, rows, model // halves), F32),
                pltpu.VMEM((halves, n, rows, model // halves), F32),
                dma((experts,)), dma((experts,)), dma((n,)), dma((n,)), dma((n,)), dma((n,)), dma((n,)), dma((n,)),
                dma((halves, n)), dma((halves, n))],
            compiler_params=pltpu.CompilerParams(collective_id=1, has_side_effects=True,
                                                 vmem_limit_bytes=VMEM_LIMIT),
        )(x2, h2, expert_idx.reshape(1, -1), w_router.T, w_in, w_out)
        return out, unflat(nk), unflat(nv)

    return jax.shard_map(decoder_block, mesh=mesh, in_specs=in_specs, out_specs=out_specs, check_vma=False)
```

```python
import functools
import jax
import jax.numpy as jnp
from jax import lax
from jax.experimental import pallas as pl
from jax.experimental.pallas import tpu as pltpu
from jax.sharding import PartitionSpec as P

EPSILON = 1e-6
NEG_BIG = -1e30
MESH = pl.DeviceIdType.MESH
F32 = jnp.float32
BF16 = jnp.bfloat16
CHUNK = 256
GROUP = 4
SLOTS = 24
SELF_VMEM = 16 * 1024 * 1024
CROSS_VMEM = 18 * 1024 * 1024
FFN_VMEM = 20 * 1024 * 1024

vmem = functools.partial(pl.BlockSpec, memory_space=pltpu.VMEM)
smem = functools.partial(pl.BlockSpec, memory_space=pltpu.SMEM)
hbm = functools.partial(pl.BlockSpec, memory_space=pltpu.HBM)


def rms(hid_f32, scale):
    inv = lax.rsqrt(jnp.mean(hid_f32 * hid_f32, axis=-1, keepdims=True) + EPSILON)
    return (hid_f32 * inv * scale.reshape(1, -1)).astype(BF16)


def dot_nn(a, b):
    return lax.dot_general(a, b, (((1,), (0,)), ((), ())), preferred_element_type=F32)


def dot_nt(a, b):
    return lax.dot_general(a, b, (((1,), (1,)), ((), ())), preferred_element_type=F32)


def remote(src, dst, send, recv, dev):
    return pltpu.make_async_remote_copy(src_ref=src, dst_ref=dst, send_sem=send, recv_sem=recv,
                                        device_id={"ws": dev}, device_id_type=MESH)


def enter(me, n):
    barrier = pltpu.get_barrier_semaphore()
    for d in range(1, n):
        pl.semaphore_signal(barrier, inc=1, device_id={"ws": lax.rem(me + d, n)}, device_id_type=MESH)
    pl.semaphore_wait(barrier, n - 1)


def rows_of(ref, i, rows):
    return ref.at[pl.ds(pl.multiple_of(i * rows, rows), rows)]


def head_mask(heads_pad, width, head_dim):
    sub = lax.broadcasted_iota(jnp.int32, (heads_pad, width), 0) * head_dim
    lane = lax.broadcasted_iota(jnp.int32, (heads_pad, width), 1)
    return (lane >= sub) & (lane < sub + head_dim)


def softmax_rows(s):
    e = jnp.exp(s - jnp.max(s, axis=-1, keepdims=True))
    return e * (1.0 / jnp.sum(e, axis=-1, keepdims=True))


def self_kernel(n, heads, pos_ref, hid_ref, mask_ref, relb_ref, ln1_ref, ln2_ref, wq_ref, wk_ref, wv_ref,
                wo_ref, wqc_ref, woc_ref, sk_ref, sv_ref, ck_ref, cv_ref,
                qc_out, h1_out, lens_out, woc_out, kbuf, vbuf, khead, vhead,
                hall, stage, got, wqkv, wall, q_s, k_s, v_s, kt_s, vt_s, qbd, snew, ctx_s, relrev,
                lsem, ksem, vsem, chsem, hsend, hrecv, asend, arecv, wsend, wrecv, fsend, frecv, lsend, lrecv):
    me = lax.axis_index("ws")
    rows, model = hid_ref.shape
    cols = wq_ref.shape[0]
    width = cols * n
    cache_len = sk_ref.shape[2]
    heads_pad = qbd.shape[0] // rows
    head_dim = width // heads
    chips = n // 2

    locals_ = [pltpu.make_async_copy(w, wqkv.at[i], lsem.at[i]) for i, w in enumerate((wq_ref, wk_ref, wv_ref))]
    locals_ += [pltpu.make_async_copy(w, rows_of(wall.at[i], me, cols), lsem.at[3 + i])
                for i, w in enumerate((wo_ref, wqc_ref, woc_ref))]
    for copy in locals_:
        copy.start()
    for b in range(rows):
        pltpu.make_async_copy(sk_ref.at[b], kbuf.at[b], ksem.at[b]).start()
        pltpu.make_async_copy(sv_ref.at[b], vbuf.at[b], vsem.at[b]).start()
    heads_of = [pltpu.make_async_copy(src.at[:, :, pl.ds(0, CHUNK)], dst, chsem.at[i])
                for i, (src, dst) in enumerate(((ck_ref, khead), (cv_ref, vhead)))]
    for copy in heads_of:
        copy.start()

    stage[...] = jnp.zeros_like(stage)
    enter(me, n)

    def h_copy(src, dev):
        return remote(hid_ref, rows_of(hall, src, rows), hsend.at[dev], hrecv.at[src], dev)

    for d in range(1, n):
        h_copy(me, lax.rem(me + d, n)).start()

    chip, core = me // 2, lax.rem(me, 2)
    def w_copy(t, src, dev):
        piece = rows_of(wall.at[t], src, cols)
        return remote(piece, piece, wsend.at[t, dev], wrecv.at[t, src], dev)

    def f_copy(t, src, dev):
        piece = rows_of(wall.at[t], src, cols)
        return remote(piece, piece, fsend.at[t, src], frecv.at[t, src], dev)

    def across(d):
        return lax.rem(chip + d, chips) * 2 + core

    half = cols // 2
    right, left, far, partner = across(1), across(3), across(2), me + 1 - 2 * core

    def l_copy(t, side, src, dev):
        piece = wall.at[t].at[pl.ds(pl.multiple_of(src * cols + side * half, half), half)]
        return remote(piece, piece, lsend.at[t, side], lrecv.at[t, side], dev)

    def w_start(t):
        for dev in (right, left, partner):
            w_copy(t, me, dev).start()

    def w_relay(t):
        w_copy(t, left, me).wait_recv()
        l_copy(t, 0, left, right).start()
        f_copy(t, left, partner).start()
        w_copy(t, right, me).wait_recv()
        l_copy(t, 1, right, left).start()
        f_copy(t, right, partner).start()

    def w_forward(t):
        for side in range(2):
            l_copy(t, side, far, me).wait_recv()
        f_copy(t, far, partner).start()

    def w_finish(t):
        w_copy(t, partner, me).wait_recv()
        for d in range(1, chips):
            f_copy(t, across(d) + 1 - 2 * core, me).wait_recv()

    for copy in locals_:
        copy.wait()
    w_start(0)
    hall[pl.ds(pl.multiple_of(me * rows, rows), rows), :] = hid_ref[...]

    rb = relb_ref[...]
    rev = (lax.broadcasted_iota(jnp.int32, (cache_len, cache_len), 0)
           + lax.broadcasted_iota(jnp.int32, (cache_len, cache_len), 1) == cache_len - 1).astype(BF16)
    hi = rb.astype(BF16)
    mid = (rb - hi.astype(F32)).astype(BF16)
    low = (rb - hi.astype(F32) - mid.astype(F32)).astype(BF16)
    relrev[...] = jnp.zeros_like(relrev)
    relrev[0:heads, :] = dot_nn(hi, rev) + dot_nn(mid, rev) + dot_nn(low, rev)
    lens_out[...] = jnp.broadcast_to(
        jnp.sum(mask_ref[...].astype(F32), axis=-1, keepdims=True), lens_out.shape).astype(jnp.int32)

    for d in range(1, n):
        h_copy(lax.rem(me + n - d, n), me).wait_recv()
    x = rms(hall[...].astype(F32), ln1_ref[...])
    for i in range(3):
        y = dot_nt(x, wqkv[i]).astype(BF16)
        for j in range(n):
            stage[j, :, i * 128:i * 128 + cols] = y[j * rows:(j + 1) * rows, :]

    def a_copy(src, dev):
        return remote(stage.at[dev], got.at[src], asend.at[dev], arecv.at[src], dev)

    for d in range(1, n):
        a_copy(me, lax.rem(me + d, n)).start()
    got[me] = stage[me]
    w_start(1)
    w_start(2)
    for d in range(1, n):
        a_copy(lax.rem(me + n - d, n), me).wait_recv()

    lane = lax.broadcasted_iota(jnp.int32, (rows, 128), 1)
    for i, dst in enumerate((q_s, k_s, v_s)):
        tiles = [None] * (width // 128)
        for s in range(n):
            piece = got[s, :, i * 128:(i + 1) * 128].astype(F32)
            t, r = divmod(s * cols, 128)
            if r:
                piece = pltpu.roll(piece, r, axis=1)
            ends = ((t, r, min(128, r + cols)), (t + 1, 0, r + cols - 128))
            for tile, lo, hi_ in ends:
                if hi_ > lo:
                    base = jnp.zeros((rows, 128), F32) if tiles[tile] is None else tiles[tile]
                    tiles[tile] = jnp.where((lane >= lo) & (lane < hi_), piece, base)
        for t, tile in enumerate(tiles):
            dst[:, t * 128:(t + 1) * 128] = tile
    diag = head_mask(heads_pad, width, head_dim)
    for b in range(rows):
        qbd[b * heads_pad:(b + 1) * heads_pad, :] = jnp.where(
            diag, jnp.broadcast_to(q_s[b:b + 1, :], diag.shape), 0.0).astype(BF16)
    cross = dot_nt(qbd[...], k_s[...].astype(BF16))
    own = (lax.broadcasted_iota(jnp.int32, cross.shape, 0) // heads_pad
           == lax.broadcasted_iota(jnp.int32, cross.shape, 1))
    snew[...] = jnp.broadcast_to(jnp.sum(jnp.where(own, cross, 0.0), axis=-1, keepdims=True), snew.shape)
    for src, dst in ((k_s, kt_s), (v_s, vt_s)):
        flipped = jnp.transpose(src[...])
        for i in range(rows // 4):
            dst[i] = flipped[:, i * 4:(i + 1) * 4]

    col = lax.broadcasted_iota(jnp.int32, (heads_pad, cache_len), 1)
    lane16 = lax.broadcasted_iota(jnp.int32, (16, cache_len), 1)

    def insert(buf, b, here, new):
        wide = jnp.broadcast_to(new, (width, 128)).astype(BF16).reshape(width // 16, 16, 128)
        for t in range(cache_len // 128):
            part = slice(t * 128, (t + 1) * 128)
            old = buf[b, :, part].reshape(width // 16, 16, 128)
            buf[b, :, part] = jnp.where(here[None, :, part], wide, old).reshape(width, 128)

    w_relay(0)

    def quad(i, carry):
        rows4 = [i * 4 + r for r in range(4)]
        head_rows = [pl.ds(pl.multiple_of(b * heads_pad, heads_pad), heads_pad) for b in rows4]
        for b in rows4:
            pltpu.make_async_copy(sk_ref.at[b], kbuf.at[b], ksem.at[b]).wait()
            pltpu.make_async_copy(sv_ref.at[b], vbuf.at[b], vsem.at[b]).wait()
        raw = [dot_nn(qbd[hr, :], kbuf[b]) for b, hr in zip(rows4, head_rows)]
        olds, news = [], []
        for s, b, hr in zip(raw, rows4, head_rows):
            pos = pos_ref[b]
            s = jnp.where(col == pos, snew[hr, 0:1], s)
            bias = pltpu.roll(relrev[...], lax.rem(pos + 1, cache_len), axis=1)
            p = softmax_rows(jnp.where(col <= pos, s + bias, NEG_BIG)).astype(BF16).astype(F32)
            news.append(jnp.sum(jnp.where(col == pos, p, 0.0), axis=-1, keepdims=True))
            olds.append(jnp.where(col == pos, 0.0, p).astype(BF16))
        outs = [dot_nt(p, vbuf[b]) for p, b in zip(olds, rows4)]
        for c, pnew, b in zip(outs, news, rows4):
            c = c + pnew * v_s[pl.ds(b, 1), :]
            ctx_s[pl.ds(b, 1), :] = jnp.sum(jnp.where(diag, c, 0.0), axis=0, keepdims=True)
        for r, b in enumerate(rows4):
            here = lane16 == pos_ref[b]
            insert(kbuf, b, here, kt_s[i, :, r:r + 1])
            insert(vbuf, b, here, vt_s[i, :, r:r + 1])

        @pl.when(i < 2)
        def _():
            w_relay(i + 1)

        @pl.when(i < 3)
        def _():
            w_forward(i)

        return carry

    lax.fori_loop(0, rows // 4, quad, 0)

    w_finish(0)
    h1 = (hid_ref[...].astype(F32) + dot_nt(ctx_s[...].astype(BF16), wall[0])).astype(BF16)
    h1_out[...] = h1
    w_finish(1)
    x = rms(h1.astype(F32), ln2_ref[...])
    qc_out[...] = dot_nt(x, wall[1])
    w_finish(2)
    woc_out[...] = wall[2]
    for copy in heads_of:
        copy.wait()

    for d in range(1, n):
        h_copy(me, lax.rem(me + d, n)).wait_send()
        a_copy(me, lax.rem(me + d, n)).wait_send()
    for t in range(3):
        for dev in (right, left, partner):
            w_copy(t, me, dev).wait_send()
        for src in (right, left, far):
            f_copy(t, src, partner).wait_send()
        l_copy(t, 0, left, right).wait_send()
        l_copy(t, 1, right, left).wait_send()


def cross_kernel(heads, lens_ref, qc_ref, h1_ref, ln3_ref, woc_ref, kbuf, vbuf, khead, vhead, ck_ref, cv_ref,
                 h2_out, x2_out, nk_out, nv_out,
                 ring, scores, probs, qbd, qf_s, ctx_s, item_row, item_col,
                 rsem, kout, vout):
    rows, width = qc_ref.shape
    src_len = ck_ref.shape[2]
    heads_pad = qbd.shape[1]
    head_dim = width // heads
    cap = item_row.shape[0]
    diag = head_mask(heads_pad, width, head_dim)

    total = 0
    for b in range(rows):
        count = (lens_ref[b, 0] - 1) // CHUNK
        for c in range(src_len // CHUNK - 1):
            @pl.when(c < count)
            def _(b=b, c=c, at=total + c):
                item_row[at] = b
                item_col[at] = c + 1

        total = total + count
    groups = (total + GROUP - 1) // GROUP
    padded = groups * GROUP

    def fill(i, carry):
        item_row[i] = rows
        item_col[i] = 0
        return carry

    lax.fori_loop(total, padded, fill, 0)

    def fetch(s):
        slot = lax.rem(s, SLOTS)

        def start(src, i):
            b = jnp.minimum(item_row[i], rows - 1)
            c = pl.multiple_of(item_col[i] * CHUNK, CHUNK)
            pltpu.make_async_copy(src.at[b, :, pl.ds(c, CHUNK)], ring.at[slot], rsem.at[slot]).start()

        @pl.when(s < padded)
        def _():
            start(ck_ref, s)

        @pl.when((s >= padded) & (s < 2 * padded))
        def _():
            start(cv_ref, s - padded)

    def arrive(s):
        slot = lax.rem(s, SLOTS)
        pltpu.make_async_copy(ck_ref.at[0, :, pl.ds(0, CHUNK)], ring.at[slot], rsem.at[slot]).wait()
        return slot

    lax.fori_loop(0, SLOTS, lambda s, c: (fetch(s), c)[1], 0)
    for b in range(rows):
        pltpu.make_async_copy(kbuf.at[b], nk_out.at[b], kout.at[b]).start()

    qf_s[...] = qc_ref[...]
    for b in range(rows):
        qbd[b] = jnp.where(diag, jnp.broadcast_to(qf_s[b:b + 1, :], diag.shape), 0.0).astype(BF16)
    qbd[rows] = jnp.zeros_like(qbd[rows])
    ctx_s[...] = jnp.zeros_like(ctx_s)

    def score_head(i, carry):
        for r in range(GROUP):
            b = i * GROUP + r
            scores[b, :, 0:CHUNK] = dot_nn(qbd[b], khead[b])
        return carry

    lax.fori_loop(0, rows // GROUP, score_head, 0)

    def group_items(base, g):
        slots = [arrive(base + g * GROUP + r) for r in range(GROUP)]
        items = [g * GROUP + r for r in range(GROUP)]
        return [(s, item_row[i], pl.multiple_of(item_col[i] * CHUNK, CHUNK)) for s, i in zip(slots, items)]

    def score_group(g, carry):
        items = group_items(0, g)
        outs = [dot_nn(qbd[b], ring[slot]) for slot, b, c in items]
        for o, (slot, b, c) in zip(outs, items):
            scores[b, :, pl.ds(c, CHUNK)] = o
        for r in range(GROUP):
            fetch(g * GROUP + r + SLOTS)
        return carry

    lax.fori_loop(0, groups, score_group, 0)

    col = lax.broadcasted_iota(jnp.int32, (heads_pad, src_len), 1)

    def soft(i, carry):
        for r in range(4):
            b = i * 4 + r
            s = jnp.where(col < lens_ref[b, 0], scores[b], NEG_BIG)
            probs[b] = softmax_rows(s).astype(BF16)
        return carry

    lax.fori_loop(0, rows // 4, soft, 0)
    probs[rows] = jnp.zeros_like(probs[rows])

    for b in range(rows):
        pltpu.make_async_copy(vbuf.at[b], nv_out.at[b], vout.at[b]).start()

    def fold(full):
        return jnp.sum(jnp.where(diag, full, 0.0), axis=0, keepdims=True)

    def value_head(i, carry):
        outs = [dot_nt(probs[i * GROUP + r, :, 0:CHUNK], vhead[i * GROUP + r]) for r in range(GROUP)]
        for r in range(GROUP):
            ctx_s[pl.ds(i * GROUP + r, 1), :] = fold(outs[r])
        return carry

    lax.fori_loop(0, rows // GROUP, value_head, 0)

    def value_group(g, carry):
        items = group_items(padded, g)
        outs = [dot_nt(probs[b, :, pl.ds(c, CHUNK)], ring[slot]) for slot, b, c in items]
        for o, (slot, b, c) in zip(outs, items):
            ctx_s[pl.ds(b, 1), :] = ctx_s[pl.ds(b, 1), :] + fold(o)
        for r in range(GROUP):
            fetch(padded + g * GROUP + r + SLOTS)
        return carry

    lax.fori_loop(0, groups, value_group, 0)

    h1 = h1_ref[...].astype(F32)
    h2 = (h1 + dot_nt(ctx_s[0:rows, :].astype(BF16), woc_ref[...])).astype(BF16)
    h2_out[...] = h2
    x2_out[...] = rms(h2.astype(F32), ln3_ref[...])
    for b in range(rows):
        pltpu.make_async_copy(kbuf.at[b], nk_out.at[b], kout.at[b]).wait()
        pltpu.make_async_copy(vbuf.at[b], nv_out.at[b], vout.at[b]).wait()


def ffn_kernel(n, x2_ref, h2_ref, idx_ref, router_ref, win_ref, wout_ref, out_ref,
               xall, idx_s, iall, rall, win, wout, act, stage, got,
               isem, osem, xsend, xrecv, jsend, jrecv, rsend, rrecv, ysend, yrecv):
    me = lax.axis_index("ws")
    rows, model = x2_ref.shape
    experts, _, hidden = win_ref.shape
    group = rows * n
    capacity = (2 * group + experts - 1) // experts

    for e in range(experts):
        pltpu.make_async_copy(win_ref.at[e], win.at[e], isem.at[e]).start()
    for e in range(experts):
        pltpu.make_async_copy(wout_ref.at[e], rows_of(wout, e, hidden), osem.at[e]).start()

    eye = (lax.broadcasted_iota(jnp.int32, (rows, rows), 0) == lax.broadcasted_iota(jnp.int32, (rows, rows), 1))
    idx_col = jnp.sum(jnp.where(eye, jnp.broadcast_to(idx_ref[...].astype(F32), (rows, rows)), 0.0),
                      axis=-1, keepdims=True)
    idx_s[...] = jnp.broadcast_to(idx_col, idx_s.shape)
    enter(me, n)

    def x_copy(src, dev):
        return remote(x2_ref, rows_of(xall, src, rows), xsend.at[dev], xrecv.at[src], dev)

    def i_copy(src, dev):
        return remote(idx_s, rows_of(iall, src, rows), jsend.at[dev], jrecv.at[src], dev)

    def r_copy(src, dev):
        return remote(router_ref, rall.at[src], rsend.at[dev], rrecv.at[src], dev)

    for copy in (x_copy, i_copy, r_copy):
        for d in range(1, n):
            copy(me, lax.rem(me + d, n)).start()
    mine = pl.ds(pl.multiple_of(me * rows, rows), rows)
    xall[mine, :] = x2_ref[...]
    iall[mine, :] = idx_s[...]
    rall[me] = router_ref[...]
    for copy in (x_copy, i_copy, r_copy):
        for d in range(1, n):
            copy(lax.rem(me + n - d, n), me).wait_recv()

    x = xall[...]
    chosen = iall[:, 0:1]
    for e in range(experts):
        pltpu.make_async_copy(win_ref.at[e], win.at[e], isem.at[e]).wait()
        u = jnp.maximum(dot_nn(x, win[e]), 0.0)
        act[:, e * hidden:(e + 1) * hidden] = jnp.where(chosen == float(e), u, 0.0).astype(BF16)
    for e in range(experts):
        pltpu.make_async_copy(wout_ref.at[e], rows_of(wout, e, hidden), osem.at[e]).wait()

    halves, _, _, span = stage.shape

    def y_copy(h, src, dev):
        return remote(stage.at[h, dev], got.at[h, src], ysend.at[h, dev], yrecv.at[h, src], dev)

    for h in range(halves):
        y = dot_nn(act[...], wout[:, h * span:(h + 1) * span])
        for j in range(n):
            stage[h, j] = y[j * rows:(j + 1) * rows, :]
        for d in range(1, n):
            y_copy(h, me, lax.rem(me + d, n)).start()
        got[h, me] = stage[h, me]

    xr = x2_ref[...].astype(F32)
    logits = [jnp.sum(xr * rall[e], axis=-1, keepdims=True) for e in range(experts)]
    top = functools.reduce(jnp.maximum, logits)
    exps = [jnp.exp(v - top) for v in logits]
    denom = functools.reduce(jnp.add, exps)
    my_idx = idx_s[:, 0:1]
    gate = functools.reduce(jnp.add, [jnp.where(my_idx == float(e), exps[e] / denom, 0.0) for e in range(experts)])
    others = jnp.transpose(iall[...])[0:rows, :]
    row = me * rows + lax.broadcasted_iota(jnp.int32, (rows, group), 0)
    col = lax.broadcasted_iota(jnp.int32, (rows, group), 1)
    slot = jnp.sum(jnp.where((others == my_idx) & (col < row), 1.0, 0.0), axis=-1, keepdims=True)
    gate = jnp.where(slot < float(capacity), gate, 0.0)

    for h in range(halves):
        for d in range(1, n):
            y_copy(h, lax.rem(me + n - d, n), me).wait_recv()
        y = functools.reduce(jnp.add, [got[h, s] for s in range(n)]).astype(BF16).astype(F32)
        part = slice(h * span, (h + 1) * span)
        out_ref[:, part] = (h2_ref[:, part].astype(F32) + y * gate).astype(BF16)

    for d in range(1, n):
        dev = lax.rem(me + d, n)
        for copy in (x_copy, i_copy, r_copy):
            copy(me, dev).wait_send()
        for h in range(halves):
            y_copy(h, me, dev).wait_send()


def solution(mesh):
    n = mesh.shape['ws']
    row_axes = ('dp', 'ws')
    row_vec = P(row_axes)
    row_mat = P(row_axes, None)
    cache_spec = P(row_axes, None, None, None)
    col_split = P(None, 'ws')
    in_specs = (row_mat, cache_spec, cache_spec, cache_spec, cache_spec, row_vec, row_mat, P(None, None), row_vec,
                P(None), P(None), P(None), col_split, col_split, col_split, col_split, col_split, col_split,
                col_split, P(None, None, 'ws'), P(None, 'ws', None))
    out_specs = (row_mat, cache_spec, cache_spec)
    dma = pltpu.SemaphoreType.DMA

    def decoder_block(hidden, self_k, self_v, cross_k, cross_v, positions, enc_mask, rel_bias, expert_idx,
                      ln_self, ln_cross, ln_ffn, wq_self, wk_self, wv_self, wo_self, wq_cross, wo_cross,
                      w_router, w_in, w_out):
        rows, model = hidden.shape
        _, heads, cache_len, head_dim = self_k.shape
        src_len = cross_k.shape[2]
        width = heads * head_dim
        cols = wq_self.shape[1]
        heads_pad = (heads + 15) // 16 * 16
        experts, _, ff = w_in.shape

        def flat(cache):
            return jnp.swapaxes(cache, 2, 3).reshape(rows, width, cache.shape[2])

        def unflat(cache):
            return jnp.swapaxes(cache.reshape(rows, heads, head_dim, cache.shape[2]), 2, 3)

        sds = jax.ShapeDtypeStruct
        sk, sv, ck, cv = flat(self_k), flat(self_v), flat(cross_k), flat(cross_v)
        def stay(x):
            return pltpu.with_memory_space_constraint(x, pltpu.HBM)

        head_shape = (rows, width, CHUNK)
        qc, h1, lens, woc, ku, vu, kh, vh = pl.pallas_call(
            functools.partial(self_kernel, n, heads),
            name="self_attention",
            out_shape=(sds((rows, width), F32), sds((rows, model), BF16), sds((rows, 128), jnp.int32),
                       pltpu.VMEM((model, width), BF16), pltpu.VMEM(sk.shape, BF16), pltpu.VMEM(sv.shape, BF16),
                       pltpu.VMEM(head_shape, BF16), pltpu.VMEM(head_shape, BF16)),
            in_specs=[smem()] + [vmem()] * 5 + [hbm()] * 10,
            out_specs=tuple([vmem()] * 8),
            scratch_shapes=[
                pltpu.VMEM((rows * n, model), BF16), pltpu.VMEM((n, rows, 384), BF16),
                pltpu.VMEM((n, rows, 384), BF16), pltpu.VMEM((3, cols, model), BF16), pltpu.VMEM((3, width, model), BF16),
                pltpu.VMEM((rows, width), F32), pltpu.VMEM((rows, width), F32), pltpu.VMEM((rows, width), F32),
                pltpu.VMEM((rows // 4, width, 4), F32), pltpu.VMEM((rows // 4, width, 4), F32),
                pltpu.VMEM((rows * heads_pad, width), BF16), pltpu.VMEM((rows * heads_pad, 128), F32),
                pltpu.VMEM((rows, width), F32), pltpu.VMEM((heads_pad, cache_len), F32),
                dma((6,)), dma((rows,)), dma((rows,)), dma((2,)), dma((n,)), dma((n,)), dma((n,)), dma((n,)),
                dma((3, n)), dma((3, n)), dma((3, n)), dma((3, n)), dma((3, 2)), dma((3, 2))],
            compiler_params=pltpu.CompilerParams(collective_id=0, has_side_effects=True,
                                                 vmem_limit_bytes=SELF_VMEM),
        )(*(stay(x) for x in (positions, hidden, enc_mask, rel_bias, ln_self, ln_cross,
                             wq_self.T, wk_self.T, wv_self.T, wo_self.T, wq_cross.T, wo_cross.T, sk, sv, ck, cv)))

        items = rows * (src_len // CHUNK) + GROUP
        h2, x2, nk, nv = pl.pallas_call(
            functools.partial(cross_kernel, heads),
            name="cross_attention",
            out_shape=(sds((rows, model), BF16), sds((rows, model), BF16), sds(sk.shape, BF16), sds(sv.shape, BF16)),
            in_specs=[smem()] + [vmem()] * 8 + [hbm()] * 2,
            out_specs=(vmem(), vmem(), hbm(), hbm()),
            scratch_shapes=[
                pltpu.VMEM((SLOTS, width, CHUNK), BF16), pltpu.VMEM((rows + 1, heads_pad, src_len), F32),
                pltpu.VMEM((rows + 1, heads_pad, src_len), BF16), pltpu.VMEM((rows + 1, heads_pad, width), BF16),
                pltpu.VMEM((rows, width), F32),
                pltpu.VMEM((rows + 8, width), F32), pltpu.SMEM((items,), jnp.int32), pltpu.SMEM((items,), jnp.int32),
                dma((SLOTS,)), dma((rows,)), dma((rows,))],
            compiler_params=pltpu.CompilerParams(vmem_limit_bytes=CROSS_VMEM),
        )(lens, qc, h1, stay(ln_ffn), woc, ku, vu, kh, vh, stay(ck), stay(cv))

        halves = 2
        out = pl.pallas_call(
            functools.partial(ffn_kernel, n),
            name="switch_ffn",
            out_shape=sds((rows, model), BF16),
            in_specs=[vmem()] * 4 + [hbm(), hbm()],
            out_specs=vmem(),
            scratch_shapes=[
                pltpu.VMEM((rows * n, model), BF16), pltpu.VMEM((rows, 128), F32), pltpu.VMEM((rows * n, 128), F32),
                pltpu.VMEM((n, 1, model), F32), pltpu.VMEM(w_in.shape, BF16), pltpu.VMEM((experts * w_out.shape[1], model), BF16),
                pltpu.VMEM((rows * n, experts * ff), BF16), pltpu.VMEM((halves, n, rows, model // halves), F32),
                pltpu.VMEM((halves, n, rows, model // halves), F32),
                dma((experts,)), dma((experts,)), dma((n,)), dma((n,)), dma((n,)), dma((n,)), dma((n,)), dma((n,)),
                dma((halves, n)), dma((halves, n))],
            compiler_params=pltpu.CompilerParams(collective_id=1, has_side_effects=True,
                                                 vmem_limit_bytes=FFN_VMEM),
        )(x2, h2, stay(expert_idx.reshape(1, -1)), stay(w_router.T), stay(w_in), stay(w_out))
        return out, unflat(nk), unflat(nv)

    return jax.shard_map(decoder_block, mesh=mesh, in_specs=in_specs, out_specs=out_specs, check_vma=False)
```

```python
import functools
import jax
import jax.numpy as jnp
from jax import lax
from jax.experimental import pallas as pl
from jax.experimental.pallas import tpu as pltpu
from jax.sharding import PartitionSpec as P

EPSILON = 1e-6
NEG_BIG = -1e30
MESH = pl.DeviceIdType.MESH
F32 = jnp.float32
BF16 = jnp.bfloat16
CHUNK = 256
GROUP = 4
SLOTS = 24
SELF_VMEM = 16 * 1024 * 1024
CROSS_VMEM = 18 * 1024 * 1024
FFN_VMEM = 20 * 1024 * 1024

vmem = functools.partial(pl.BlockSpec, memory_space=pltpu.VMEM)
smem = functools.partial(pl.BlockSpec, memory_space=pltpu.SMEM)
hbm = functools.partial(pl.BlockSpec, memory_space=pltpu.HBM)


def rms(hid_f32, scale):
    inv = lax.rsqrt(jnp.mean(hid_f32 * hid_f32, axis=-1, keepdims=True) + EPSILON)
    return (hid_f32 * inv * scale.reshape(1, -1)).astype(BF16)


def dot_nn(a, b):
    return lax.dot_general(a, b, (((1,), (0,)), ((), ())), preferred_element_type=F32)


def dot_nt(a, b):
    return lax.dot_general(a, b, (((1,), (1,)), ((), ())), preferred_element_type=F32)


def remote(src, dst, send, recv, dev):
    return pltpu.make_async_remote_copy(src_ref=src, dst_ref=dst, send_sem=send, recv_sem=recv,
                                        device_id={"ws": dev}, device_id_type=MESH)


def enter(me, n):
    barrier = pltpu.get_barrier_semaphore()
    for d in range(1, n):
        pl.semaphore_signal(barrier, inc=1, device_id={"ws": lax.rem(me + d, n)}, device_id_type=MESH)
    pl.semaphore_wait(barrier, n - 1)


def rows_of(ref, i, rows):
    return ref.at[pl.ds(pl.multiple_of(i * rows, rows), rows)]


def head_mask(heads_pad, width, head_dim):
    sub = lax.broadcasted_iota(jnp.int32, (heads_pad, width), 0) * head_dim
    lane = lax.broadcasted_iota(jnp.int32, (heads_pad, width), 1)
    return (lane >= sub) & (lane < sub + head_dim)


def softmax_rows(s):
    e = jnp.exp(s - jnp.max(s, axis=-1, keepdims=True))
    return e * (1.0 / jnp.sum(e, axis=-1, keepdims=True))


def self_kernel(n, heads, pos_ref, hid_ref, mask_ref, relb_ref, ln1_ref, ln2_ref, wq_ref, wk_ref, wv_ref,
                wo_ref, wqc_ref, woc_ref, sk_ref, sv_ref, ck_ref, cv_ref,
                qc_out, h1_out, lens_out, woc_out, kbuf, vbuf, khead, vhead,
                hall, stage, got, wqkv, wall, q_s, k_s, v_s, kt_s, vt_s, qbd, snew, ctx_s, relrev,
                lsem, ksem, vsem, chsem, hsend, hrecv, asend, arecv, wsend, wrecv, fsend, frecv, lsend, lrecv):
    me = lax.axis_index("ws")
    rows, model = hid_ref.shape
    cols = wq_ref.shape[0]
    width = cols * n
    cache_len = sk_ref.shape[2]
    heads_pad = qbd.shape[0] // rows
    head_dim = width // heads
    chips = n // 2

    locals_ = [pltpu.make_async_copy(w, wqkv.at[i], lsem.at[i]) for i, w in enumerate((wq_ref, wk_ref, wv_ref))]
    locals_ += [pltpu.make_async_copy(w, rows_of(wall.at[i], me, cols), lsem.at[3 + i])
                for i, w in enumerate((wo_ref, wqc_ref, woc_ref))]
    for copy in locals_:
        copy.start()
    heads_of = [pltpu.make_async_copy(src.at[:, :, pl.ds(0, CHUNK)], dst, chsem.at[i])
                for i, (src, dst) in enumerate(((ck_ref, khead), (cv_ref, vhead)))]

    stage[...] = jnp.zeros_like(stage)
    enter(me, n)

    def h_copy(src, dev):
        return remote(hid_ref, rows_of(hall, src, rows), hsend.at[dev], hrecv.at[src], dev)

    for d in range(1, n):
        h_copy(me, lax.rem(me + d, n)).start()
    for b in range(rows):
        pltpu.make_async_copy(sk_ref.at[b], kbuf.at[b], ksem.at[b]).start()
        pltpu.make_async_copy(sv_ref.at[b], vbuf.at[b], vsem.at[b]).start()

    chip, core = me // 2, lax.rem(me, 2)
    def w_copy(t, src, dev):
        piece = rows_of(wall.at[t], src, cols)
        return remote(piece, piece, wsend.at[t, dev], wrecv.at[t, src], dev)

    def f_copy(t, src, dev):
        piece = rows_of(wall.at[t], src, cols)
        return remote(piece, piece, fsend.at[t, src], frecv.at[t, src], dev)

    def across(d):
        return lax.rem(chip + d, chips) * 2 + core

    half = cols // 2
    right, left, far, partner = across(1), across(3), across(2), me + 1 - 2 * core

    def l_copy(t, side, src, dev):
        piece = wall.at[t].at[pl.ds(pl.multiple_of(src * cols + side * half, half), half)]
        return remote(piece, piece, lsend.at[t, side], lrecv.at[t, side], dev)

    def w_start(t):
        for dev in (right, left, partner):
            w_copy(t, me, dev).start()

    def w_relay(t):
        w_copy(t, left, me).wait_recv()
        l_copy(t, 0, left, right).start()
        f_copy(t, left, partner).start()
        w_copy(t, right, me).wait_recv()
        l_copy(t, 1, right, left).start()
        f_copy(t, right, partner).start()

    def w_forward(t):
        for side in range(2):
            l_copy(t, side, far, me).wait_recv()
        f_copy(t, far, partner).start()

    def w_finish(t):
        w_copy(t, partner, me).wait_recv()
        for d in range(1, chips):
            f_copy(t, across(d) + 1 - 2 * core, me).wait_recv()

    for copy in locals_:
        copy.wait()
    w_start(0)
    hall[pl.ds(pl.multiple_of(me * rows, rows), rows), :] = hid_ref[...]

    rb = relb_ref[...]
    rev = (lax.broadcasted_iota(jnp.int32, (cache_len, cache_len), 0)
           + lax.broadcasted_iota(jnp.int32, (cache_len, cache_len), 1) == cache_len - 1).astype(BF16)
    hi = rb.astype(BF16)
    mid = (rb - hi.astype(F32)).astype(BF16)
    low = (rb - hi.astype(F32) - mid.astype(F32)).astype(BF16)
    relrev[...] = jnp.zeros_like(relrev)
    relrev[0:heads, :] = dot_nn(hi, rev) + dot_nn(mid, rev) + dot_nn(low, rev)
    lens_out[...] = jnp.broadcast_to(
        jnp.sum(mask_ref[...].astype(F32), axis=-1, keepdims=True), lens_out.shape).astype(jnp.int32)

    for d in range(1, n):
        h_copy(lax.rem(me + n - d, n), me).wait_recv()
    x = rms(hall[...].astype(F32), ln1_ref[...])
    for i in range(3):
        y = dot_nt(x, wqkv[i]).astype(BF16)
        for j in range(n):
            stage[j, :, i * 128:i * 128 + cols] = y[j * rows:(j + 1) * rows, :]

    def a_copy(src, dev):
        return remote(stage.at[dev], got.at[src], asend.at[dev], arecv.at[src], dev)

    for d in range(1, n):
        a_copy(me, lax.rem(me + d, n)).start()
    got[me] = stage[me]
    for copy in heads_of:
        copy.start()
    w_start(1)
    w_relay(0)
    w_start(2)
    for d in range(1, n):
        a_copy(lax.rem(me + n - d, n), me).wait_recv()

    lane = lax.broadcasted_iota(jnp.int32, (rows, 128), 1)
    for i, dst in enumerate((q_s, k_s, v_s)):
        tiles = [None] * (width // 128)
        for s in range(n):
            piece = got[s, :, i * 128:(i + 1) * 128].astype(F32)
            t, r = divmod(s * cols, 128)
            if r:
                piece = pltpu.roll(piece, r, axis=1)
            ends = ((t, r, min(128, r + cols)), (t + 1, 0, r + cols - 128))
            for tile, lo, hi_ in ends:
                if hi_ > lo:
                    base = jnp.zeros((rows, 128), F32) if tiles[tile] is None else tiles[tile]
                    tiles[tile] = jnp.where((lane >= lo) & (lane < hi_), piece, base)
        for t, tile in enumerate(tiles):
            dst[:, t * 128:(t + 1) * 128] = tile
    diag = head_mask(heads_pad, width, head_dim)
    for b in range(rows):
        qbd[b * heads_pad:(b + 1) * heads_pad, :] = jnp.where(
            diag, jnp.broadcast_to(q_s[b:b + 1, :], diag.shape), 0.0).astype(BF16)
    cross = dot_nt(qbd[...], k_s[...].astype(BF16))
    own = (lax.broadcasted_iota(jnp.int32, cross.shape, 0) // heads_pad
           == lax.broadcasted_iota(jnp.int32, cross.shape, 1))
    snew[...] = jnp.broadcast_to(jnp.sum(jnp.where(own, cross, 0.0), axis=-1, keepdims=True), snew.shape)
    for src, dst in ((k_s, kt_s), (v_s, vt_s)):
        flipped = jnp.transpose(src[...])
        for i in range(rows // 4):
            dst[i] = flipped[:, i * 4:(i + 1) * 4]

    col = lax.broadcasted_iota(jnp.int32, (heads_pad, cache_len), 1)
    lane16 = lax.broadcasted_iota(jnp.int32, (16, cache_len), 1)

    def insert(buf, b, here, new):
        wide = jnp.broadcast_to(new, (width, 128)).astype(BF16).reshape(width // 16, 16, 128)
        for t in range(cache_len // 128):
            part = slice(t * 128, (t + 1) * 128)
            old = buf[b, :, part].reshape(width // 16, 16, 128)
            buf[b, :, part] = jnp.where(here[None, :, part], wide, old).reshape(width, 128)

    def quad(i, carry):
        rows4 = [i * 4 + r for r in range(4)]
        head_rows = [pl.ds(pl.multiple_of(b * heads_pad, heads_pad), heads_pad) for b in rows4]
        for b in rows4:
            pltpu.make_async_copy(sk_ref.at[b], kbuf.at[b], ksem.at[b]).wait()
            pltpu.make_async_copy(sv_ref.at[b], vbuf.at[b], vsem.at[b]).wait()
        raw = [dot_nn(qbd[hr, :], kbuf[b]) for b, hr in zip(rows4, head_rows)]
        olds, news = [], []
        for s, b, hr in zip(raw, rows4, head_rows):
            pos = pos_ref[b]
            s = jnp.where(col == pos, snew[hr, 0:1], s)
            bias = pltpu.roll(relrev[...], lax.rem(pos + 1, cache_len), axis=1)
            p = softmax_rows(jnp.where(col <= pos, s + bias, NEG_BIG)).astype(BF16).astype(F32)
            news.append(jnp.sum(jnp.where(col == pos, p, 0.0), axis=-1, keepdims=True))
            olds.append(jnp.where(col == pos, 0.0, p).astype(BF16))
        outs = [dot_nt(p, vbuf[b]) for p, b in zip(olds, rows4)]
        for c, pnew, b in zip(outs, news, rows4):
            c = c + pnew * v_s[pl.ds(b, 1), :]
            ctx_s[pl.ds(b, 1), :] = jnp.sum(jnp.where(diag, c, 0.0), axis=0, keepdims=True)
        for r, b in enumerate(rows4):
            here = lane16 == pos_ref[b]
            insert(kbuf, b, here, kt_s[i, :, r:r + 1])
            insert(vbuf, b, here, vt_s[i, :, r:r + 1])

        @pl.when(i == 0)
        def _():
            w_forward(0)

        @pl.when((i == 1) | (i == 2))
        def _():
            w_relay(i)

        return carry

    lax.fori_loop(0, rows // 4, quad, 0)

    w_forward(1)
    w_finish(0)
    h1 = (hid_ref[...].astype(F32) + dot_nt(ctx_s[...].astype(BF16), wall[0])).astype(BF16)
    h1_out[...] = h1
    w_forward(2)
    w_finish(1)
    x = rms(h1.astype(F32), ln2_ref[...])
    qc_out[...] = dot_nt(x, wall[1])
    w_finish(2)
    woc_out[...] = wall[2]
    for copy in heads_of:
        copy.wait()

    for d in range(1, n):
        h_copy(me, lax.rem(me + d, n)).wait_send()
        a_copy(me, lax.rem(me + d, n)).wait_send()
    for t in range(3):
        for dev in (right, left, partner):
            w_copy(t, me, dev).wait_send()
        for src in (right, left, far):
            f_copy(t, src, partner).wait_send()
        l_copy(t, 0, left, right).wait_send()
        l_copy(t, 1, right, left).wait_send()


def cross_kernel(heads, lens_ref, qc_ref, h1_ref, ln3_ref, woc_ref, kbuf, vbuf, khead, vhead, ck_ref, cv_ref,
                 h2_out, x2_out, nk_out, nv_out,
                 ring, scores, probs, qbd, qf_s, ctx_s, item_row, item_col,
                 rsem, kout, vout):
    rows, width = qc_ref.shape
    src_len = ck_ref.shape[2]
    heads_pad = qbd.shape[1]
    head_dim = width // heads
    cap = item_row.shape[0]
    diag = head_mask(heads_pad, width, head_dim)

    total = 0
    for b in range(rows):
        count = (lens_ref[b, 0] - 1) // CHUNK
        for c in range(src_len // CHUNK - 1):
            @pl.when(c < count)
            def _(b=b, c=c, at=total + c):
                item_row[at] = b
                item_col[at] = c + 1

        total = total + count
    groups = (total + GROUP - 1) // GROUP
    padded = groups * GROUP

    def fill(i, carry):
        item_row[i] = rows
        item_col[i] = 0
        return carry

    lax.fori_loop(total, padded, fill, 0)

    def fetch(s):
        slot = lax.rem(s, SLOTS)

        def start(src, i):
            b = jnp.minimum(item_row[i], rows - 1)
            c = pl.multiple_of(item_col[i] * CHUNK, CHUNK)
            pltpu.make_async_copy(src.at[b, :, pl.ds(c, CHUNK)], ring.at[slot], rsem.at[slot]).start()

        @pl.when(s < padded)
        def _():
            start(ck_ref, s)

        @pl.when((s >= padded) & (s < 2 * padded))
        def _():
            start(cv_ref, s - padded)

    def arrive(s):
        slot = lax.rem(s, SLOTS)
        pltpu.make_async_copy(ck_ref.at[0, :, pl.ds(0, CHUNK)], ring.at[slot], rsem.at[slot]).wait()
        return slot

    lax.fori_loop(0, SLOTS, lambda s, c: (fetch(s), c)[1], 0)
    for b in range(rows):
        pltpu.make_async_copy(kbuf.at[b], nk_out.at[b], kout.at[b]).start()

    qf_s[...] = qc_ref[...]
    for b in range(rows):
        qbd[b] = jnp.where(diag, jnp.broadcast_to(qf_s[b:b + 1, :], diag.shape), 0.0).astype(BF16)
    qbd[rows] = jnp.zeros_like(qbd[rows])
    ctx_s[...] = jnp.zeros_like(ctx_s)

    def score_head(i, carry):
        for r in range(GROUP):
            b = i * GROUP + r
            scores[b, :, 0:CHUNK] = dot_nn(qbd[b], khead[b])
        return carry

    lax.fori_loop(0, rows // GROUP, score_head, 0)

    def group_items(base, g):
        slots = [arrive(base + g * GROUP + r) for r in range(GROUP)]
        items = [g * GROUP + r for r in range(GROUP)]
        return [(s, item_row[i], pl.multiple_of(item_col[i] * CHUNK, CHUNK)) for s, i in zip(slots, items)]

    def score_group(g, carry):
        items = group_items(0, g)
        outs = [dot_nn(qbd[b], ring[slot]) for slot, b, c in items]
        for o, (slot, b, c) in zip(outs, items):
            scores[b, :, pl.ds(c, CHUNK)] = o
        for r in range(GROUP):
            fetch(g * GROUP + r + SLOTS)
        return carry

    lax.fori_loop(0, groups, score_group, 0)

    col = lax.broadcasted_iota(jnp.int32, (heads_pad, src_len), 1)

    def soft(i, carry):
        for r in range(4):
            b = i * 4 + r
            s = jnp.where(col < lens_ref[b, 0], scores[b], NEG_BIG)
            probs[b] = softmax_rows(s).astype(BF16)
        return carry

    lax.fori_loop(0, rows // 4, soft, 0)
    probs[rows] = jnp.zeros_like(probs[rows])

    for b in range(rows):
        pltpu.make_async_copy(vbuf.at[b], nv_out.at[b], vout.at[b]).start()

    def fold(full):
        return jnp.sum(jnp.where(diag, full, 0.0), axis=0, keepdims=True)

    def value_head(i, carry):
        outs = [dot_nt(probs[i * GROUP + r, :, 0:CHUNK], vhead[i * GROUP + r]) for r in range(GROUP)]
        for r in range(GROUP):
            ctx_s[pl.ds(i * GROUP + r, 1), :] = fold(outs[r])
        return carry

    lax.fori_loop(0, rows // GROUP, value_head, 0)

    def value_group(g, carry):
        items = group_items(padded, g)
        outs = [dot_nt(probs[b, :, pl.ds(c, CHUNK)], ring[slot]) for slot, b, c in items]
        for o, (slot, b, c) in zip(outs, items):
            ctx_s[pl.ds(b, 1), :] = ctx_s[pl.ds(b, 1), :] + fold(o)
        for r in range(GROUP):
            fetch(padded + g * GROUP + r + SLOTS)
        return carry

    lax.fori_loop(0, groups, value_group, 0)

    h1 = h1_ref[...].astype(F32)
    h2 = (h1 + dot_nt(ctx_s[0:rows, :].astype(BF16), woc_ref[...])).astype(BF16)
    h2_out[...] = h2
    x2_out[...] = rms(h2.astype(F32), ln3_ref[...])
    for b in range(rows):
        pltpu.make_async_copy(kbuf.at[b], nk_out.at[b], kout.at[b]).wait()
        pltpu.make_async_copy(vbuf.at[b], nv_out.at[b], vout.at[b]).wait()


def ffn_kernel(n, x2_ref, h2_ref, idx_ref, router_ref, win_ref, wout_ref, out_ref,
               xall, idx_s, iall, rall, win, wout, act, stage, pair, total, got,
               isem, osem, xsend, xrecv, jsend, jrecv, rsend, rrecv, psend, precv, ysend, yrecv):
    me = lax.axis_index("ws")
    rows, model = x2_ref.shape
    experts, _, hidden = win_ref.shape
    group = rows * n
    capacity = (2 * group + experts - 1) // experts

    eye = (lax.broadcasted_iota(jnp.int32, (rows, rows), 0) == lax.broadcasted_iota(jnp.int32, (rows, rows), 1))
    idx_col = jnp.sum(jnp.where(eye, jnp.broadcast_to(idx_ref[...].astype(F32), (rows, rows)), 0.0),
                      axis=-1, keepdims=True)
    idx_s[...] = jnp.broadcast_to(idx_col, idx_s.shape)
    enter(me, n)

    def x_copy(src, dev):
        return remote(x2_ref, rows_of(xall, src, rows), xsend.at[dev], xrecv.at[src], dev)

    def i_copy(src, dev):
        return remote(idx_s, rows_of(iall, src, rows), jsend.at[dev], jrecv.at[src], dev)

    def r_copy(src, dev):
        return remote(router_ref, rall.at[src], rsend.at[dev], rrecv.at[src], dev)

    for copy in (x_copy, i_copy, r_copy):
        for d in range(1, n):
            copy(me, lax.rem(me + d, n)).start()
    for e in range(experts):
        pltpu.make_async_copy(win_ref.at[e], win.at[e], isem.at[e]).start()
    for e in range(experts):
        pltpu.make_async_copy(wout_ref.at[e], rows_of(wout, e, hidden), osem.at[e]).start()
    mine = pl.ds(pl.multiple_of(me * rows, rows), rows)
    xall[mine, :] = x2_ref[...]
    iall[mine, :] = idx_s[...]
    rall[me] = router_ref[...]
    for copy in (x_copy, i_copy, r_copy):
        for d in range(1, n):
            copy(lax.rem(me + n - d, n), me).wait_recv()

    x = xall[...]
    chosen = iall[:, 0:1]
    for e in range(experts):
        pltpu.make_async_copy(win_ref.at[e], win.at[e], isem.at[e]).wait()
        u = jnp.maximum(dot_nn(x, win[e]), 0.0)
        act[:, e * hidden:(e + 1) * hidden] = jnp.where(chosen == float(e), u, 0.0).astype(BF16)
    for e in range(experts):
        pltpu.make_async_copy(wout_ref.at[e], rows_of(wout, e, hidden), osem.at[e]).wait()

    halves, _, chips, _, span = stage.shape
    chip, core = me // 2, lax.rem(me, 2)
    partner = me + 1 - 2 * core

    def p_copy(h):
        return remote(stage.at[h, 1 - core], pair.at[h], psend.at[h], precv.at[h], partner)

    def y_copy(h, src, dst):
        return remote(total.at[h, dst], got.at[h, src], ysend.at[h, dst], yrecv.at[h, src], dst * 2 + core)

    def send_sums(h):
        p_copy(h).wait_recv()
        total[h] = stage[h, core] + pair[h]
        for d in range(1, chips):
            y_copy(h, chip, lax.rem(chip + d, chips)).start()
        got[h, chip] = total[h, chip]

    for h in range(halves):
        y = dot_nn(act[...], wout[:, h * span:(h + 1) * span])
        for j in range(n):
            stage[h, j % 2, j // 2] = y[j * rows:(j + 1) * rows, :]
        p_copy(h).start()
        if h:
            send_sums(h - 1)
    send_sums(halves - 1)

    xr = x2_ref[...].astype(F32)
    logits = [jnp.sum(xr * rall[e], axis=-1, keepdims=True) for e in range(experts)]
    top = functools.reduce(jnp.maximum, logits)
    exps = [jnp.exp(v - top) for v in logits]
    denom = functools.reduce(jnp.add, exps)
    my_idx = idx_s[:, 0:1]
    gate = functools.reduce(jnp.add, [jnp.where(my_idx == float(e), exps[e] / denom, 0.0) for e in range(experts)])
    others = jnp.transpose(iall[...])[0:rows, :]
    row = me * rows + lax.broadcasted_iota(jnp.int32, (rows, group), 0)
    col = lax.broadcasted_iota(jnp.int32, (rows, group), 1)
    slot = jnp.sum(jnp.where((others == my_idx) & (col < row), 1.0, 0.0), axis=-1, keepdims=True)
    gate = jnp.where(slot < float(capacity), gate, 0.0)

    for h in range(halves):
        for d in range(1, chips):
            y_copy(h, lax.rem(chip + d, chips), chip).wait_recv()
        y = functools.reduce(jnp.add, [got[h, s] for s in range(chips)]).astype(BF16).astype(F32)
        part = slice(h * span, (h + 1) * span)
        out_ref[:, part] = (h2_ref[:, part].astype(F32) + y * gate).astype(BF16)

    for d in range(1, n):
        dev = lax.rem(me + d, n)
        for copy in (x_copy, i_copy, r_copy):
            copy(me, dev).wait_send()
    for h in range(halves):
        p_copy(h).wait_send()
        for d in range(1, chips):
            y_copy(h, chip, lax.rem(chip + d, chips)).wait_send()


def solution(mesh):
    n = mesh.shape['ws']
    row_axes = ('dp', 'ws')
    row_vec = P(row_axes)
    row_mat = P(row_axes, None)
    cache_spec = P(row_axes, None, None, None)
    col_split = P(None, 'ws')
    in_specs = (row_mat, cache_spec, cache_spec, cache_spec, cache_spec, row_vec, row_mat, P(None, None), row_vec,
                P(None), P(None), P(None), col_split, col_split, col_split, col_split, col_split, col_split,
                col_split, P(None, None, 'ws'), P(None, 'ws', None))
    out_specs = (row_mat, cache_spec, cache_spec)
    dma = pltpu.SemaphoreType.DMA

    def decoder_block(hidden, self_k, self_v, cross_k, cross_v, positions, enc_mask, rel_bias, expert_idx,
                      ln_self, ln_cross, ln_ffn, wq_self, wk_self, wv_self, wo_self, wq_cross, wo_cross,
                      w_router, w_in, w_out):
        rows, model = hidden.shape
        _, heads, cache_len, head_dim = self_k.shape
        src_len = cross_k.shape[2]
        width = heads * head_dim
        cols = wq_self.shape[1]
        heads_pad = (heads + 15) // 16 * 16
        experts, _, ff = w_in.shape

        def flat(cache):
            return jnp.swapaxes(cache, 2, 3).reshape(rows, width, cache.shape[2])

        def unflat(cache):
            return jnp.swapaxes(cache.reshape(rows, heads, head_dim, cache.shape[2]), 2, 3)

        sds = jax.ShapeDtypeStruct
        sk, sv, ck, cv = flat(self_k), flat(self_v), flat(cross_k), flat(cross_v)
        def stay(x):
            return pltpu.with_memory_space_constraint(x, pltpu.HBM)

        head_shape = (rows, width, CHUNK)
        qc, h1, lens, woc, ku, vu, kh, vh = pl.pallas_call(
            functools.partial(self_kernel, n, heads),
            name="self_attention",
            out_shape=(sds((rows, width), F32), sds((rows, model), BF16), sds((rows, 128), jnp.int32),
                       pltpu.VMEM((model, width), BF16), pltpu.VMEM(sk.shape, BF16), pltpu.VMEM(sv.shape, BF16),
                       pltpu.VMEM(head_shape, BF16), pltpu.VMEM(head_shape, BF16)),
            in_specs=[smem()] + [vmem()] * 5 + [hbm()] * 10,
            out_specs=tuple([vmem()] * 8),
            scratch_shapes=[
                pltpu.VMEM((rows * n, model), BF16), pltpu.VMEM((n, rows, 384), BF16),
                pltpu.VMEM((n, rows, 384), BF16), pltpu.VMEM((3, cols, model), BF16), pltpu.VMEM((3, width, model), BF16),
                pltpu.VMEM((rows, width), F32), pltpu.VMEM((rows, width), F32), pltpu.VMEM((rows, width), F32),
                pltpu.VMEM((rows // 4, width, 4), F32), pltpu.VMEM((rows // 4, width, 4), F32),
                pltpu.VMEM((rows * heads_pad, width), BF16), pltpu.VMEM((rows * heads_pad, 128), F32),
                pltpu.VMEM((rows, width), F32), pltpu.VMEM((heads_pad, cache_len), F32),
                dma((6,)), dma((rows,)), dma((rows,)), dma((2,)), dma((n,)), dma((n,)), dma((n,)), dma((n,)),
                dma((3, n)), dma((3, n)), dma((3, n)), dma((3, n)), dma((3, 2)), dma((3, 2))],
            compiler_params=pltpu.CompilerParams(collective_id=0, has_side_effects=True,
                                                 vmem_limit_bytes=SELF_VMEM),
        )(*(stay(x) for x in (positions, hidden, enc_mask, rel_bias, ln_self, ln_cross,
                             wq_self.T, wk_self.T, wv_self.T, wo_self.T, wq_cross.T, wo_cross.T, sk, sv, ck, cv)))

        items = rows * (src_len // CHUNK) + GROUP
        h2, x2, nk, nv = pl.pallas_call(
            functools.partial(cross_kernel, heads),
            name="cross_attention",
            out_shape=(sds((rows, model), BF16), sds((rows, model), BF16), sds(sk.shape, BF16), sds(sv.shape, BF16)),
            in_specs=[smem()] + [vmem()] * 8 + [hbm()] * 2,
            out_specs=(vmem(), vmem(), hbm(), hbm()),
            scratch_shapes=[
                pltpu.VMEM((SLOTS, width, CHUNK), BF16), pltpu.VMEM((rows + 1, heads_pad, src_len), F32),
                pltpu.VMEM((rows + 1, heads_pad, src_len), BF16), pltpu.VMEM((rows + 1, heads_pad, width), BF16),
                pltpu.VMEM((rows, width), F32),
                pltpu.VMEM((rows + 8, width), F32), pltpu.SMEM((items,), jnp.int32), pltpu.SMEM((items,), jnp.int32),
                dma((SLOTS,)), dma((rows,)), dma((rows,))],
            compiler_params=pltpu.CompilerParams(vmem_limit_bytes=CROSS_VMEM),
        )(lens, qc, h1, stay(ln_ffn), woc, ku, vu, kh, vh, stay(ck), stay(cv))

        halves = 3
        out = pl.pallas_call(
            functools.partial(ffn_kernel, n),
            name="switch_ffn",
            out_shape=sds((rows, model), BF16),
            in_specs=[vmem()] * 4 + [hbm(), hbm()],
            out_specs=vmem(),
            scratch_shapes=[
                pltpu.VMEM((rows * n, model), BF16), pltpu.VMEM((rows, 128), F32), pltpu.VMEM((rows * n, 128), F32),
                pltpu.VMEM((n, 1, model), F32), pltpu.VMEM(w_in.shape, BF16), pltpu.VMEM((experts * w_out.shape[1], model), BF16),
                pltpu.VMEM((rows * n, experts * ff), BF16), pltpu.VMEM((halves, 2, n // 2, rows, model // halves), F32),
                pltpu.VMEM((halves, n // 2, rows, model // halves), F32), pltpu.VMEM((halves, n // 2, rows, model // halves), F32),
                pltpu.VMEM((halves, n // 2, rows, model // halves), F32),
                dma((experts,)), dma((experts,)), dma((n,)), dma((n,)), dma((n,)), dma((n,)), dma((n,)), dma((n,)),
                dma((halves,)), dma((halves,)), dma((halves, n // 2)), dma((halves, n // 2))],
            compiler_params=pltpu.CompilerParams(collective_id=1, has_side_effects=True,
                                                 vmem_limit_bytes=FFN_VMEM),
        )(x2, h2, stay(expert_idx.reshape(1, -1)), stay(w_router.T), stay(w_in), stay(w_out))
        return out, unflat(nk), unflat(nv)

    return jax.shard_map(decoder_block, mesh=mesh, in_specs=in_specs, out_specs=out_specs, check_vma=False)
```

```python
import functools
import jax
import jax.numpy as jnp
from jax import lax
from jax.experimental import pallas as pl
from jax.experimental.pallas import tpu as pltpu
from jax.sharding import PartitionSpec as P

EPSILON = 1e-6
NEG_BIG = -1e30
MESH = pl.DeviceIdType.MESH
F32 = jnp.float32
BF16 = jnp.bfloat16
CHUNK = 256
GROUP = 4
SLOTS = 32
SELF_VMEM = 16 * 1024 * 1024
CROSS_VMEM = 21 * 1024 * 1024
FFN_VMEM = 20 * 1024 * 1024

vmem = functools.partial(pl.BlockSpec, memory_space=pltpu.VMEM)
smem = functools.partial(pl.BlockSpec, memory_space=pltpu.SMEM)
hbm = functools.partial(pl.BlockSpec, memory_space=pltpu.HBM)


def rms(hid_f32, scale):
    inv = lax.rsqrt(jnp.mean(hid_f32 * hid_f32, axis=-1, keepdims=True) + EPSILON)
    return (hid_f32 * inv * scale.reshape(1, -1)).astype(BF16)


def dot_nn(a, b):
    return lax.dot_general(a, b, (((1,), (0,)), ((), ())), preferred_element_type=F32)


def dot_nt(a, b):
    return lax.dot_general(a, b, (((1,), (1,)), ((), ())), preferred_element_type=F32)


def remote(src, dst, send, recv, dev):
    return pltpu.make_async_remote_copy(src_ref=src, dst_ref=dst, send_sem=send, recv_sem=recv,
                                        device_id={"ws": dev}, device_id_type=MESH)


def far_first(n):
    return sorted(range(1, n), key=lambda d: abs(d - n // 2))


def enter(me, n):
    barrier = pltpu.get_barrier_semaphore()
    for d in range(1, n):
        pl.semaphore_signal(barrier, inc=1, device_id={"ws": lax.rem(me + d, n)}, device_id_type=MESH)
    pl.semaphore_wait(barrier, n - 1)


def rows_of(ref, i, rows):
    return ref.at[pl.ds(pl.multiple_of(i * rows, rows), rows)]


def group_gather(me, n, rows, own, buf, send, recv):
    core = lax.rem(me, 2)
    flip = 1 - 2 * core
    partner = me + flip
    peers = [lax.rem(me + 2 * d, n) for d in range(1, n // 2)]

    def direct(dev, src):
        return remote(own, rows_of(buf, src, rows), send.at[dev], recv.at[src], dev)

    def passed(src):
        piece = rows_of(buf, src, rows)
        return remote(piece, piece, send.at[src + flip], recv.at[src], partner)

    def start():
        for dev in (*peers, partner):
            direct(dev, me).start()

    def finish():
        for src in peers:
            direct(me, src).wait_recv()
            passed(src).start()
        direct(me, partner).wait_recv()
        for src in peers:
            passed(src + flip).wait_recv()

    def drain():
        for dev in (*peers, partner):
            direct(dev, me).wait_send()
        for src in peers:
            passed(src).wait_send()

    return start, finish, drain


def head_mask(heads_pad, width, head_dim):
    sub = lax.broadcasted_iota(jnp.int32, (heads_pad, width), 0) * head_dim
    lane = lax.broadcasted_iota(jnp.int32, (heads_pad, width), 1)
    return (lane >= sub) & (lane < sub + head_dim)


def softmax_rows(s):
    e = jnp.exp(s - jnp.max(s, axis=-1, keepdims=True))
    return e * (1.0 / jnp.sum(e, axis=-1, keepdims=True))


def self_kernel(n, heads, pos_ref, hid_ref, mask_ref, relb_ref, ln1_ref, ln2_ref, wq_ref, wk_ref, wv_ref,
                wo_ref, wqc_ref, woc_ref, sk_ref, sv_ref, ck_ref, cv_ref,
                qc_out, h1_out, lens_out, woc_out, kbuf, vbuf, khead, vhead,
                hall, stage, got, wqkv, wall, q_s, k_s, v_s, kt_s, vt_s, qbd, snew, ctx_s, relrev,
                lsem, ksem, vsem, chsem, hsend, hrecv, asend, arecv, wsend, wrecv, fsend, frecv, lsend, lrecv):
    me = lax.axis_index("ws")
    rows, model = hid_ref.shape
    cols = wq_ref.shape[0]
    width = cols * n
    cache_len = sk_ref.shape[2]
    heads_pad = qbd.shape[0] // rows
    head_dim = width // heads
    chips = n // 2

    locals_ = [pltpu.make_async_copy(w, wqkv.at[i], lsem.at[i]) for i, w in enumerate((wq_ref, wk_ref, wv_ref))]
    locals_ += [pltpu.make_async_copy(w, rows_of(wall.at[i], me, cols), lsem.at[3 + i])
                for i, w in enumerate((wo_ref, wqc_ref, woc_ref))]
    for copy in locals_:
        copy.start()
    heads_of = [pltpu.make_async_copy(src.at[:, :, pl.ds(0, CHUNK)], dst, chsem.at[i])
                for i, (src, dst) in enumerate(((ck_ref, khead), (cv_ref, vhead)))]

    stage[...] = jnp.zeros_like(stage)
    enter(me, n)

    h_start, h_finish, h_drain = group_gather(me, n, rows, hid_ref, hall, hsend, hrecv)
    h_start()
    for b in range(rows):
        pltpu.make_async_copy(sk_ref.at[b], kbuf.at[b], ksem.at[b]).start()
        pltpu.make_async_copy(sv_ref.at[b], vbuf.at[b], vsem.at[b]).start()

    chip, core = me // 2, lax.rem(me, 2)
    def w_copy(t, src, dev):
        piece = rows_of(wall.at[t], src, cols)
        return remote(piece, piece, wsend.at[t, dev], wrecv.at[t, src], dev)

    def f_copy(t, src, dev):
        piece = rows_of(wall.at[t], src, cols)
        return remote(piece, piece, fsend.at[t, src], frecv.at[t, src], dev)

    def across(d):
        return lax.rem(chip + d, chips) * 2 + core

    half = cols // 2
    right, left, far, partner = across(1), across(3), across(2), me + 1 - 2 * core

    def l_copy(t, side, src, dev):
        piece = wall.at[t].at[pl.ds(pl.multiple_of(src * cols + side * half, half), half)]
        return remote(piece, piece, lsend.at[t, side], lrecv.at[t, side], dev)

    def w_start(t):
        for dev in (right, left, partner):
            w_copy(t, me, dev).start()

    def w_relay(t):
        w_copy(t, left, me).wait_recv()
        l_copy(t, 0, left, right).start()
        f_copy(t, left, partner).start()
        w_copy(t, right, me).wait_recv()
        l_copy(t, 1, right, left).start()
        f_copy(t, right, partner).start()

    def w_forward(t):
        for side in range(2):
            l_copy(t, side, far, me).wait_recv()
        f_copy(t, far, partner).start()

    def w_finish(t):
        w_copy(t, partner, me).wait_recv()
        for d in range(1, chips):
            f_copy(t, across(d) + 1 - 2 * core, me).wait_recv()

    for copy in locals_:
        copy.wait()
    w_start(0)
    hall[pl.ds(pl.multiple_of(me * rows, rows), rows), :] = hid_ref[...]

    rb = relb_ref[...]
    rev = (lax.broadcasted_iota(jnp.int32, (cache_len, cache_len), 0)
           + lax.broadcasted_iota(jnp.int32, (cache_len, cache_len), 1) == cache_len - 1).astype(BF16)
    hi = rb.astype(BF16)
    mid = (rb - hi.astype(F32)).astype(BF16)
    low = (rb - hi.astype(F32) - mid.astype(F32)).astype(BF16)
    relrev[...] = jnp.zeros_like(relrev)
    relrev[0:heads, :] = dot_nn(hi, rev) + dot_nn(mid, rev) + dot_nn(low, rev)
    lens_out[...] = jnp.broadcast_to(
        jnp.sum(mask_ref[...].astype(F32), axis=-1, keepdims=True), lens_out.shape).astype(jnp.int32)

    h_finish()
    x = rms(hall[...].astype(F32), ln1_ref[...])
    for i in range(3):
        y = dot_nt(x, wqkv[i]).astype(BF16)
        for j in range(n):
            stage[j, :, i * 128:i * 128 + cols] = y[j * rows:(j + 1) * rows, :]

    def a_copy(src, dev):
        return remote(stage.at[dev], got.at[src], asend.at[dev], arecv.at[src], dev)

    for d in far_first(n):
        a_copy(me, lax.rem(me + d, n)).start()
    got[me] = stage[me]
    for copy in heads_of:
        copy.start()
    w_start(1)
    w_relay(0)
    w_start(2)
    for d in range(1, n):
        a_copy(lax.rem(me + n - d, n), me).wait_recv()

    lane = lax.broadcasted_iota(jnp.int32, (rows, 128), 1)
    for i, dst in enumerate((q_s, k_s, v_s)):
        tiles = [None] * (width // 128)
        for s in range(n):
            piece = got[s, :, i * 128:(i + 1) * 128].astype(F32)
            t, r = divmod(s * cols, 128)
            if r:
                piece = pltpu.roll(piece, r, axis=1)
            ends = ((t, r, min(128, r + cols)), (t + 1, 0, r + cols - 128))
            for tile, lo, hi_ in ends:
                if hi_ > lo:
                    base = jnp.zeros((rows, 128), F32) if tiles[tile] is None else tiles[tile]
                    tiles[tile] = jnp.where((lane >= lo) & (lane < hi_), piece, base)
        for t, tile in enumerate(tiles):
            dst[:, t * 128:(t + 1) * 128] = tile
    diag = head_mask(heads_pad, width, head_dim)
    for b in range(rows):
        qbd[b * heads_pad:(b + 1) * heads_pad, :] = jnp.where(
            diag, jnp.broadcast_to(q_s[b:b + 1, :], diag.shape), 0.0).astype(BF16)
    cross = dot_nt(qbd[...], k_s[...].astype(BF16))
    own = (lax.broadcasted_iota(jnp.int32, cross.shape, 0) // heads_pad
           == lax.broadcasted_iota(jnp.int32, cross.shape, 1))
    snew[...] = jnp.broadcast_to(jnp.sum(jnp.where(own, cross, 0.0), axis=-1, keepdims=True), snew.shape)
    for src, dst in ((k_s, kt_s), (v_s, vt_s)):
        flipped = jnp.transpose(src[...])
        for i in range(rows // 4):
            dst[i] = flipped[:, i * 4:(i + 1) * 4]

    col = lax.broadcasted_iota(jnp.int32, (heads_pad, cache_len), 1)
    lane16 = lax.broadcasted_iota(jnp.int32, (16, cache_len), 1)

    def insert(buf, b, here, new):
        wide = jnp.broadcast_to(new, (width, 128)).astype(BF16).reshape(width // 16, 16, 128)
        for t in range(cache_len // 128):
            part = slice(t * 128, (t + 1) * 128)
            old = buf[b, :, part].reshape(width // 16, 16, 128)
            buf[b, :, part] = jnp.where(here[None, :, part], wide, old).reshape(width, 128)

    def quad(i, carry):
        rows4 = [i * 4 + r for r in range(4)]
        head_rows = [pl.ds(pl.multiple_of(b * heads_pad, heads_pad), heads_pad) for b in rows4]
        for b in rows4:
            pltpu.make_async_copy(sk_ref.at[b], kbuf.at[b], ksem.at[b]).wait()
            pltpu.make_async_copy(sv_ref.at[b], vbuf.at[b], vsem.at[b]).wait()
        raw = [dot_nn(qbd[hr, :], kbuf[b]) for b, hr in zip(rows4, head_rows)]
        olds, news = [], []
        for s, b, hr in zip(raw, rows4, head_rows):
            pos = pos_ref[b]
            s = jnp.where(col == pos, snew[hr, 0:1], s)
            bias = pltpu.roll(relrev[...], lax.rem(pos + 1, cache_len), axis=1)
            p = softmax_rows(jnp.where(col <= pos, s + bias, NEG_BIG)).astype(BF16).astype(F32)
            news.append(jnp.sum(jnp.where(col == pos, p, 0.0), axis=-1, keepdims=True))
            olds.append(jnp.where(col == pos, 0.0, p).astype(BF16))
        outs = [dot_nt(p, vbuf[b]) for p, b in zip(olds, rows4)]
        for c, pnew, b in zip(outs, news, rows4):
            c = c + pnew * v_s[pl.ds(b, 1), :]
            ctx_s[pl.ds(b, 1), :] = jnp.sum(jnp.where(diag, c, 0.0), axis=0, keepdims=True)
        for r, b in enumerate(rows4):
            here = lane16 == pos_ref[b]
            insert(kbuf, b, here, kt_s[i, :, r:r + 1])
            insert(vbuf, b, here, vt_s[i, :, r:r + 1])

        @pl.when(i == 0)
        def _():
            w_relay(1)

        @pl.when(i == 1)
        def _():
            w_forward(0)

        @pl.when(i == 2)
        def _():
            w_relay(2)

        return carry

    lax.fori_loop(0, rows // 4, quad, 0)

    w_forward(1)
    w_finish(0)
    h1 = (hid_ref[...].astype(F32) + dot_nt(ctx_s[...].astype(BF16), wall[0])).astype(BF16)
    h1_out[...] = h1
    w_forward(2)
    w_finish(1)
    x = rms(h1.astype(F32), ln2_ref[...])
    qc_out[...] = dot_nt(x, wall[1])
    w_finish(2)
    woc_out[...] = wall[2]
    for copy in heads_of:
        copy.wait()

    for d in range(1, n):
        a_copy(me, lax.rem(me + d, n)).wait_send()
    h_drain()
    for t in range(3):
        for dev in (right, left, partner):
            w_copy(t, me, dev).wait_send()
        for src in (right, left, far):
            f_copy(t, src, partner).wait_send()
        l_copy(t, 0, left, right).wait_send()
        l_copy(t, 1, right, left).wait_send()


def cross_kernel(heads, lens_ref, qc_ref, h1_ref, ln3_ref, woc_ref, kbuf, vbuf, khead, vhead, ck_ref, cv_ref,
                 h2_out, x2_out, nk_out, nv_out,
                 ring, scores, probs, qbd, qf_s, ctx_s, item_row, item_col,
                 rsem, kout, vout):
    rows, width = qc_ref.shape
    src_len = ck_ref.shape[2]
    heads_pad = qbd.shape[1]
    head_dim = width // heads
    cap = item_row.shape[0]
    diag = head_mask(heads_pad, width, head_dim)

    total = 0
    for b in range(rows):
        count = (lens_ref[b, 0] - 1) // CHUNK
        for c in range(src_len // CHUNK - 1):
            @pl.when(c < count)
            def _(b=b, c=c, at=total + c):
                item_row[at] = b
                item_col[at] = c + 1

        total = total + count
    groups = (total + GROUP - 1) // GROUP
    padded = groups * GROUP

    def fill(i, carry):
        item_row[i] = rows
        item_col[i] = 0
        return carry

    lax.fori_loop(total, padded, fill, 0)

    def fetch(s):
        slot = lax.rem(s, SLOTS)

        def start(src, i):
            b = jnp.minimum(item_row[i], rows - 1)
            c = pl.multiple_of(item_col[i] * CHUNK, CHUNK)
            pltpu.make_async_copy(src.at[b, :, pl.ds(c, CHUNK)], ring.at[slot], rsem.at[slot]).start()

        @pl.when(s < padded)
        def _():
            start(ck_ref, s)

        @pl.when((s >= padded) & (s < 2 * padded))
        def _():
            start(cv_ref, s - padded)

    def arrive(s):
        slot = lax.rem(s, SLOTS)
        pltpu.make_async_copy(ck_ref.at[0, :, pl.ds(0, CHUNK)], ring.at[slot], rsem.at[slot]).wait()
        return slot

    lax.fori_loop(0, SLOTS, lambda s, c: (fetch(s), c)[1], 0)
    for b in range(rows):
        pltpu.make_async_copy(kbuf.at[b], nk_out.at[b], kout.at[b]).start()

    qf_s[...] = qc_ref[...]
    for b in range(rows):
        qbd[b] = jnp.where(diag, jnp.broadcast_to(qf_s[b:b + 1, :], diag.shape), 0.0).astype(BF16)
    qbd[rows] = jnp.zeros_like(qbd[rows])
    ctx_s[...] = jnp.zeros_like(ctx_s)

    def score_head(i, carry):
        for r in range(GROUP):
            b = i * GROUP + r
            scores[b, :, 0:CHUNK] = dot_nn(qbd[b], khead[b])
        return carry

    lax.fori_loop(0, rows // GROUP, score_head, 0)

    def group_items(base, g):
        slots = [arrive(base + g * GROUP + r) for r in range(GROUP)]
        items = [g * GROUP + r for r in range(GROUP)]
        return [(s, item_row[i], pl.multiple_of(item_col[i] * CHUNK, CHUNK)) for s, i in zip(slots, items)]

    def score_group(g, carry):
        items = group_items(0, g)
        outs = [dot_nn(qbd[b], ring[slot]) for slot, b, c in items]
        for o, (slot, b, c) in zip(outs, items):
            scores[b, :, pl.ds(c, CHUNK)] = o
        for r in range(GROUP):
            fetch(g * GROUP + r + SLOTS)
        return carry

    lax.fori_loop(0, groups, score_group, 0)

    col = lax.broadcasted_iota(jnp.int32, (heads_pad, src_len), 1)

    def soft(i, carry):
        for r in range(4):
            b = i * 4 + r
            s = jnp.where(col < lens_ref[b, 0], scores[b], NEG_BIG)
            probs[b] = softmax_rows(s).astype(BF16)
        return carry

    lax.fori_loop(0, rows // 4, soft, 0)
    probs[rows] = jnp.zeros_like(probs[rows])

    for b in range(rows):
        pltpu.make_async_copy(vbuf.at[b], nv_out.at[b], vout.at[b]).start()

    def fold(full):
        return jnp.sum(jnp.where(diag, full, 0.0), axis=0, keepdims=True)

    def value_head(i, carry):
        outs = [dot_nt(probs[i * GROUP + r, :, 0:CHUNK], vhead[i * GROUP + r]) for r in range(GROUP)]
        for r in range(GROUP):
            ctx_s[pl.ds(i * GROUP + r, 1), :] = fold(outs[r])
        return carry

    lax.fori_loop(0, rows // GROUP, value_head, 0)

    def value_group(g, carry):
        items = group_items(padded, g)
        outs = [dot_nt(probs[b, :, pl.ds(c, CHUNK)], ring[slot]) for slot, b, c in items]
        for o, (slot, b, c) in zip(outs, items):
            ctx_s[pl.ds(b, 1), :] = ctx_s[pl.ds(b, 1), :] + fold(o)
        for r in range(GROUP):
            fetch(padded + g * GROUP + r + SLOTS)
        return carry

    lax.fori_loop(0, groups, value_group, 0)

    h1 = h1_ref[...].astype(F32)
    h2 = (h1 + dot_nt(ctx_s[0:rows, :].astype(BF16), woc_ref[...])).astype(BF16)
    h2_out[...] = h2
    x2_out[...] = rms(h2.astype(F32), ln3_ref[...])
    for b in range(rows):
        pltpu.make_async_copy(kbuf.at[b], nk_out.at[b], kout.at[b]).wait()
        pltpu.make_async_copy(vbuf.at[b], nv_out.at[b], vout.at[b]).wait()


def ffn_kernel(n, x2_ref, h2_ref, idx_ref, router_ref, win_ref, wout_ref, out_ref,
               xall, idx_s, iall, rall, win, wout, act, stage, pair, total, got,
               isem, osem, xsend, xrecv, jsend, jrecv, rsend, rrecv, psend, precv, ysend, yrecv):
    me = lax.axis_index("ws")
    rows, model = x2_ref.shape
    experts, _, hidden = win_ref.shape
    group = rows * n
    capacity = (2 * group + experts - 1) // experts

    eye = (lax.broadcasted_iota(jnp.int32, (rows, rows), 0) == lax.broadcasted_iota(jnp.int32, (rows, rows), 1))
    idx_col = jnp.sum(jnp.where(eye, jnp.broadcast_to(idx_ref[...].astype(F32), (rows, rows)), 0.0),
                      axis=-1, keepdims=True)
    idx_s[...] = jnp.broadcast_to(idx_col, idx_s.shape).astype(BF16)
    enter(me, n)

    def x_copy(src, dev):
        return remote(x2_ref, rows_of(xall, src, rows), xsend.at[dev], xrecv.at[src], dev)

    def i_copy(src, dev):
        return remote(idx_s, rows_of(iall, src, rows), jsend.at[dev], jrecv.at[src], dev)

    def r_copy(src, dev):
        return remote(router_ref, rall.at[src], rsend.at[dev], rrecv.at[src], dev)

    for copy in (x_copy, i_copy, r_copy):
        for d in far_first(n):
            copy(me, lax.rem(me + d, n)).start()
    for e in range(experts):
        pltpu.make_async_copy(win_ref.at[e], win.at[e], isem.at[e]).start()
    for e in range(experts):
        pltpu.make_async_copy(wout_ref.at[e], rows_of(wout, e, hidden), osem.at[e]).start()
    mine = pl.ds(pl.multiple_of(me * rows, rows), rows)
    xall[mine, :] = x2_ref[...]
    iall[mine, :] = idx_s[...]
    rall[me] = router_ref[...]
    for copy in (x_copy, i_copy):
        for d in range(1, n):
            copy(lax.rem(me + n - d, n), me).wait_recv()

    x = xall[...]
    chosen = iall[...].astype(F32)[:, 0:1]
    for e in range(experts):
        pltpu.make_async_copy(win_ref.at[e], win.at[e], isem.at[e]).wait()
        u = jnp.maximum(dot_nn(x, win[e]), 0.0)
        act[:, e * hidden:(e + 1) * hidden] = jnp.where(chosen == float(e), u, 0.0).astype(BF16)
    for e in range(experts):
        pltpu.make_async_copy(wout_ref.at[e], rows_of(wout, e, hidden), osem.at[e]).wait()

    halves, _, chips, _, span = stage.shape
    chip, core = me // 2, lax.rem(me, 2)
    partner = me + 1 - 2 * core

    def p_copy(h):
        return remote(stage.at[h, 1 - core], pair.at[h], psend.at[h], precv.at[h], partner)

    def y_copy(h, src, dst):
        return remote(total.at[h, dst], got.at[h, src], ysend.at[h, dst], yrecv.at[h, src], dst * 2 + core)

    def send_sums(h):
        p_copy(h).wait_recv()
        total[h] = stage[h, core] + pair[h]
        for d in range(1, chips):
            y_copy(h, chip, lax.rem(chip + d, chips)).start()
        got[h, chip] = total[h, chip]

    for h in range(halves):
        y = dot_nn(act[...], wout[:, h * span:(h + 1) * span])
        for j in range(n):
            stage[h, j % 2, j // 2] = y[j * rows:(j + 1) * rows, :]
        p_copy(h).start()
        if h:
            send_sums(h - 1)
    send_sums(halves - 1)

    for d in range(1, n):
        r_copy(lax.rem(me + n - d, n), me).wait_recv()
    xr = x2_ref[...].astype(F32)
    logits = [jnp.sum(xr * rall[e], axis=-1, keepdims=True) for e in range(experts)]
    top = functools.reduce(jnp.maximum, logits)
    exps = [jnp.exp(v - top) for v in logits]
    denom = functools.reduce(jnp.add, exps)
    my_idx = idx_s[...].astype(F32)[:, 0:1]
    gate = functools.reduce(jnp.add, [jnp.where(my_idx == float(e), exps[e] / denom, 0.0) for e in range(experts)])
    others = jnp.transpose(iall[...].astype(F32))[0:rows, :]
    row = me * rows + lax.broadcasted_iota(jnp.int32, (rows, group), 0)
    col = lax.broadcasted_iota(jnp.int32, (rows, group), 1)
    slot = jnp.sum(jnp.where((others == my_idx) & (col < row), 1.0, 0.0), axis=-1, keepdims=True)
    gate = jnp.where(slot < float(capacity), gate, 0.0)

    for h in range(halves):
        for d in range(1, chips):
            y_copy(h, lax.rem(chip + d, chips), chip).wait_recv()
        y = functools.reduce(jnp.add, [got[h, s] for s in range(chips)]).astype(BF16).astype(F32)
        part = slice(h * span, (h + 1) * span)
        out_ref[:, part] = (h2_ref[:, part].astype(F32) + y * gate).astype(BF16)

    for d in range(1, n):
        dev = lax.rem(me + d, n)
        for copy in (x_copy, i_copy, r_copy):
            copy(me, dev).wait_send()
    for h in range(halves):
        p_copy(h).wait_send()
        for d in range(1, chips):
            y_copy(h, chip, lax.rem(chip + d, chips)).wait_send()


def solution(mesh):
    n = mesh.shape['ws']
    row_axes = ('dp', 'ws')
    row_vec = P(row_axes)
    row_mat = P(row_axes, None)
    cache_spec = P(row_axes, None, None, None)
    col_split = P(None, 'ws')
    in_specs = (row_mat, cache_spec, cache_spec, cache_spec, cache_spec, row_vec, row_mat, P(None, None), row_vec,
                P(None), P(None), P(None), col_split, col_split, col_split, col_split, col_split, col_split,
                col_split, P(None, None, 'ws'), P(None, 'ws', None))
    out_specs = (row_mat, cache_spec, cache_spec)
    dma = pltpu.SemaphoreType.DMA

    def decoder_block(hidden, self_k, self_v, cross_k, cross_v, positions, enc_mask, rel_bias, expert_idx,
                      ln_self, ln_cross, ln_ffn, wq_self, wk_self, wv_self, wo_self, wq_cross, wo_cross,
                      w_router, w_in, w_out):
        rows, model = hidden.shape
        _, heads, cache_len, head_dim = self_k.shape
        src_len = cross_k.shape[2]
        width = heads * head_dim
        cols = wq_self.shape[1]
        heads_pad = (heads + 15) // 16 * 16
        experts, _, ff = w_in.shape

        def flat(cache):
            return jnp.swapaxes(cache, 2, 3).reshape(rows, width, cache.shape[2])

        def unflat(cache):
            return jnp.swapaxes(cache.reshape(rows, heads, head_dim, cache.shape[2]), 2, 3)

        sds = jax.ShapeDtypeStruct
        sk, sv, ck, cv = flat(self_k), flat(self_v), flat(cross_k), flat(cross_v)
        def stay(x):
            return pltpu.with_memory_space_constraint(x, pltpu.HBM)

        head_shape = (rows, width, CHUNK)
        qc, h1, lens, woc, ku, vu, kh, vh = pl.pallas_call(
            functools.partial(self_kernel, n, heads),
            name="self_attention",
            out_shape=(sds((rows, width), F32), sds((rows, model), BF16), sds((rows, 128), jnp.int32),
                       pltpu.VMEM((model, width), BF16), pltpu.VMEM(sk.shape, BF16), pltpu.VMEM(sv.shape, BF16),
                       pltpu.VMEM(head_shape, BF16), pltpu.VMEM(head_shape, BF16)),
            in_specs=[smem()] + [vmem()] * 5 + [hbm()] * 10,
            out_specs=tuple([vmem()] * 8),
            scratch_shapes=[
                pltpu.VMEM((rows * n, model), BF16), pltpu.VMEM((n, rows, 384), BF16),
                pltpu.VMEM((n, rows, 384), BF16), pltpu.VMEM((3, cols, model), BF16), pltpu.VMEM((3, width, model), BF16),
                pltpu.VMEM((rows, width), F32), pltpu.VMEM((rows, width), F32), pltpu.VMEM((rows, width), F32),
                pltpu.VMEM((rows // 4, width, 4), F32), pltpu.VMEM((rows // 4, width, 4), F32),
                pltpu.VMEM((rows * heads_pad, width), BF16), pltpu.VMEM((rows * heads_pad, 128), F32),
                pltpu.VMEM((rows, width), F32), pltpu.VMEM((heads_pad, cache_len), F32),
                dma((6,)), dma((rows,)), dma((rows,)), dma((2,)), dma((n,)), dma((n,)), dma((n,)), dma((n,)),
                dma((3, n)), dma((3, n)), dma((3, n)), dma((3, n)), dma((3, 2)), dma((3, 2))],
            compiler_params=pltpu.CompilerParams(collective_id=0, has_side_effects=True,
                                                 vmem_limit_bytes=SELF_VMEM),
        )(*(stay(x) for x in (positions, hidden, enc_mask, rel_bias, ln_self, ln_cross,
                             wq_self.T, wk_self.T, wv_self.T, wo_self.T, wq_cross.T, wo_cross.T, sk, sv, ck, cv)))

        items = rows * (src_len // CHUNK) + GROUP
        h2, x2, nk, nv = pl.pallas_call(
            functools.partial(cross_kernel, heads),
            name="cross_attention",
            out_shape=(sds((rows, model), BF16), sds((rows, model), BF16), sds(sk.shape, BF16), sds(sv.shape, BF16)),
            in_specs=[smem()] + [vmem()] * 8 + [hbm()] * 2,
            out_specs=(vmem(), vmem(), hbm(), hbm()),
            scratch_shapes=[
                pltpu.VMEM((SLOTS, width, CHUNK), BF16), pltpu.VMEM((rows + 1, heads_pad, src_len), F32),
                pltpu.VMEM((rows + 1, heads_pad, src_len), BF16), pltpu.VMEM((rows + 1, heads_pad, width), BF16),
                pltpu.VMEM((rows, width), F32),
                pltpu.VMEM((rows + 8, width), F32), pltpu.SMEM((items,), jnp.int32), pltpu.SMEM((items,), jnp.int32),
                dma((SLOTS,)), dma((rows,)), dma((rows,))],
            compiler_params=pltpu.CompilerParams(vmem_limit_bytes=CROSS_VMEM),
        )(lens, qc, h1, stay(ln_ffn), woc, ku, vu, kh, vh, stay(ck), stay(cv))

        halves = 3
        out = pl.pallas_call(
            functools.partial(ffn_kernel, n),
            name="switch_ffn",
            out_shape=sds((rows, model), BF16),
            in_specs=[vmem()] * 4 + [hbm(), hbm()],
            out_specs=vmem(),
            scratch_shapes=[
                pltpu.VMEM((rows * n, model), BF16), pltpu.VMEM((rows, 128), BF16), pltpu.VMEM((rows * n, 128), BF16),
                pltpu.VMEM((n, 1, model), F32), pltpu.VMEM(w_in.shape, BF16), pltpu.VMEM((experts * w_out.shape[1], model), BF16),
                pltpu.VMEM((rows * n, experts * ff), BF16), pltpu.VMEM((halves, 2, n // 2, rows, model // halves), F32),
                pltpu.VMEM((halves, n // 2, rows, model // halves), F32), pltpu.VMEM((halves, n // 2, rows, model // halves), F32),
                pltpu.VMEM((halves, n // 2, rows, model // halves), F32),
                dma((experts,)), dma((experts,)), dma((n,)), dma((n,)), dma((n,)), dma((n,)), dma((n,)), dma((n,)),
                dma((halves,)), dma((halves,)), dma((halves, n // 2)), dma((halves, n // 2))],
            compiler_params=pltpu.CompilerParams(collective_id=1, has_side_effects=True,
                                                 vmem_limit_bytes=FFN_VMEM),
        )(x2, h2, stay(expert_idx.reshape(1, -1)), stay(w_router.T), stay(w_in), stay(w_out))
        return out, unflat(nk), unflat(nv)

    return jax.shard_map(decoder_block, mesh=mesh, in_specs=in_specs, out_specs=out_specs, check_vma=False)
```
